32 devices in a mesh: img: 4 (over x, core), rows: 8 (over z, y).
Axes of the slice: x: 2, y: 2, z: 4, core: 2. Of those that a mesh axis runs over, the one named last changes fastest.
Arguments:
- feat_fine: bfloat16 [256, 128, 256], P(('img', 'rows')), parts along dimension 0, may hold values from -6 to 6
- feat_second: bfloat16 [128, 64, 256], P(('img', 'rows')), parts along dimension 0, may hold values from -6 to 6
- feat_third: bfloat16 [64, 32, 256], P(('img', 'rows')), parts along dimension 0, may hold values from -6 to 6
- conv_weight: bfloat16 [10, 9, 256, 256], replicated, may hold values from -0.125 to 0.125
- conv_bias: float32 [10, 256], replicated, may hold values from -3 to 3
- out_weight: bfloat16 [3, 256, 256], replicated, may hold values from -0.375 to 0.375
- out_bias: float32 [3, 256], replicated, may hold values from -3 to 3
Outputs:
- joined: bfloat16 [512, 256, 256], P(('img', 'rows')), parts along dimension 0
The draws below stay inside these ranges and needn't reach their ends.
There are 4 independent parts, one for each index of `img`. The reference program is written for one: setup_inputs(seed, part) draws one part's arguments, and reference() takes and returns one part's arrays. A program takes and returns all parts, laid end to end along the dimension named above; an argument that names none is the same for every part. Nothing has to cross between parts.
All inputs are finite; a program needn't handle non-finite values.
Results may differ from the reference program's by a relative error of at most 0.015.
Values may be sent and summed in bfloat16 or wider, within the bound.
A program may use at most 128 MiB of HBM per device.

```python
import jax
import jax.numpy as jnp
from jax import lax

CH = 256
BASE_COLS = 32
HEIGHT = 16


def steps_of(key, extent, split, least, largest):
    gain = 1.0
    for dim, shards_of in split:
        steps = jax.random.uniform(jax.random.fold_in(jax.random.fold_in(key, 6), dim), (shards_of,), jnp.float32, least / len(split), largest / len(split))
        gain = gain * jnp.repeat(jnp.exp(steps), extent[dim] // shards_of).reshape((-1,) + (1,) * (len(extent) - 1 - dim))
    return gain


def gaussian(own_key, shape, width, limit, pieces=(), kind=jnp.bfloat16):
    values = width * jax.random.normal(own_key, shape, jnp.float32)
    if pieces:
        values = values * steps_of(own_key, shape, pieces, -0.22, 0.18)
    return jnp.clip(values, -limit, limit).astype(kind)


def setup_inputs(seed: int = 0, part: int = 0) -> dict:
    key_list = jax.random.split(jax.random.key(seed), 8)
    own_keys = jax.random.split(jax.random.fold_in(key_list[7], part), 8)
    feat_fine = gaussian(own_keys[0], (4 * HEIGHT, 4 * BASE_COLS, CH), 1.0, 6.0, ((0, 8),))
    feat_second = gaussian(own_keys[1], (2 * HEIGHT, 2 * BASE_COLS, CH), 1.0, 6.0, ((0, 8),))
    feat_third = gaussian(own_keys[2], (HEIGHT, BASE_COLS, CH), 1.0, 6.0, ((0, 8),))
    conv_weight = gaussian(key_list[3], (10, 9, CH, CH), (9 * CH) ** -0.5, 0.125)
    conv_bias = gaussian(key_list[4], (10, CH), 0.5, 3.0, (), jnp.float32)
    out_weight = gaussian(key_list[5], (3, CH, CH), CH ** -0.5, 0.375)
    out_bias = gaussian(key_list[6], (3, CH), 0.5, 3.0, (), jnp.float32)
    return dict(feat_fine=feat_fine, feat_second=feat_second, feat_third=feat_third, conv_weight=conv_weight, conv_bias=conv_bias, out_weight=out_weight, out_bias=out_bias)


def conv_full(source, weight, addend):
    height, columns, channels = source.shape
    padded = jnp.pad(source, ((1, 1), (1, 1), (0, 0)))
    summed = jnp.zeros((height * columns, weight.shape[2]), jnp.float32)
    for offset in range(9):
        window = padded[offset // 3:offset // 3 + height, offset % 3:offset % 3 + columns, :]
        summed = summed + jnp.dot(window.reshape(height * columns, channels), weight[offset], preferred_element_type=jnp.float32)
    return summed.reshape(height, columns, -1) + addend


def residual_unit(source, conv_weight, conv_bias, first):
    hidden = jax.nn.relu(conv_full(jax.nn.relu(source), conv_weight[first], conv_bias[first])).astype(jnp.bfloat16)
    return conv_full(hidden, conv_weight[first + 1], conv_bias[first + 1]) + source.astype(jnp.float32)


def interp_matrix(first_out, count_out, first_in, count_in, size_in):
    outputs = first_out + jnp.arange(count_out, dtype=jnp.int32)
    lowest = (outputs + 1) // 2 - 1
    parity = (outputs % 2).astype(jnp.float32)
    weight_hi = 0.25 + 0.5 * (1.0 - parity)
    low_index = jnp.clip(lowest, 0, size_in - 1).astype(jnp.int32)
    high_index = jnp.clip(lowest + 1, 0, size_in - 1).astype(jnp.int32)
    inputs = first_in + jnp.arange(count_in, dtype=jnp.int32)
    at_low = (inputs[None, :] == low_index[:, None]).astype(jnp.float32)
    at_high = (inputs[None, :] == high_index[:, None]).astype(jnp.float32)
    return (1.0 - weight_hi)[:, None] * at_low + weight_hi[:, None] * at_high


def upsample(source, row_table, col_table):
    rows_in, columns, channels = source.shape
    segmented = jnp.dot(row_table, source.astype(jnp.float32).reshape(rows_in, columns * channels), precision=lax.Precision.HIGHEST)
    segmented = segmented.reshape(-1, columns, channels)
    return jnp.einsum("jw,awc->ajc", col_table, segmented, precision=lax.Precision.HIGHEST).astype(jnp.bfloat16)


def project(lifted, weight, addend):
    flat = lifted.reshape(-1, lifted.shape[2])
    result = jnp.dot(flat, weight, preferred_element_type=jnp.float32) + addend
    return result.astype(jnp.bfloat16).reshape(lifted.shape)


def refine(path, out_weight, out_bias, level):
    rows_in, columns, channels = path.shape
    row_table = interp_matrix(0, 2 * rows_in, 0, rows_in, rows_in)
    col_table = interp_matrix(0, 2 * columns, 0, columns, columns)
    return project(upsample(path, row_table, col_table), out_weight[level], out_bias[level])


def reference(feat_fine, feat_second, feat_third, conv_weight, conv_bias, out_weight, out_bias):
    path = residual_unit(feat_third, conv_weight, conv_bias, 0).astype(jnp.bfloat16)
    path = refine(path, out_weight, out_bias, 0)
    segments = ((feat_second, 2, 1), (feat_fine, 6, 2))
    for feature, first, level in segments:
        merged = (residual_unit(feature, conv_weight, conv_bias, first) + path.astype(jnp.float32)).astype(jnp.bfloat16)
        path = residual_unit(merged, conv_weight, conv_bias, first + 2).astype(jnp.bfloat16)
        path = refine(path, out_weight, out_bias, level)
    return path
```

```python
import functools

import jax
import jax.numpy as jnp
from jax import lax
from jax.experimental import pallas as pl
from jax.experimental.pallas import tpu as pltpu
from jax.sharding import PartitionSpec as P

MESH = pl.DeviceIdType.MESH
LANES = 16
VMEM_MIB = 44
FINE, SECOND, THIRD = 0, 1, 2
HALOS = (5, 6, 5)
WEIGHT_ORDER = (6, 0, 1, 2, 3, 4, 5, 7, 8, 9)


def direct_sends(blocks):
    plan = []
    for level in (THIRD, SECOND, FINE):
        block, halo = blocks[level], HALOS[level]
        for distance in range(1, -(-halo // block) + 1):
            if level == THIRD or distance > 1:
                plan.append((level, distance, min(block, halo - (distance - 1) * block)))
    return plan


def pair_chunks(level, block):
    near = min(block, HALOS[level])
    lead = near - near // 2 if level == FINE else near
    cuts = ((0, lead), (lead, near), (near, block))
    return [(a, block - b, b - a, b <= near) for a, b in cuts if b > a]


def edge_steps(values, clamp):
    steps = values.shape[1]
    first, last = values[:, 0], values[:, steps - 1]
    place = lax.broadcasted_iota(jnp.int32, first.shape, 1)
    zero = jnp.zeros_like(first)
    before = jnp.where(place == 0, first if clamp else zero, pltpu.roll(last, 1, 1))
    after = jnp.where(place == LANES - 1, last if clamp else zero, pltpu.roll(first, LANES - 1, 1))
    return before, after


def kernel(
    devices, fine_hbm, second_hbm, third_hbm, conv_hbm, bias_hbm, proj_hbm, proj_bias_hbm, lines_f, table,
    fine_ref, second_ref, third_ref, bias_ref, proj_bias_ref,
    fine_up, fine_down, second_up, second_down, third_up, third_down,
    fine_peer, fine_far, second_peer, second_far, fine_x, second_x, third_x, stage,
    weights, projs, padded_f, hidden_f, merged_f, path_f, padded_s, hidden_s, merged_s, path_s,
    padded_t, hidden_t, refined_f, refined_s, refined_t, proj_y,
    up_send, up_recv, down_send, down_recv,
    pair_send, pair_recv, far_send, far_recv, weight_sem, proj_sem, in_sem,
):
    me = lax.axis_index("rows")
    own = (fine_ref, second_ref, third_ref)
    ups = (fine_up, second_up, third_up)
    downs = (fine_down, second_down, third_down)
    blocks = tuple(ref.shape[0] for ref in own)
    plan = direct_sends(blocks)
    fields = (fine_x, second_x, third_x)
    peers = (fine_peer, second_peer)
    fars = (fine_far, second_far)
    odd = me % 2
    even = odd == 0
    partner = me + 1 - 2 * odd
    target = me + 2 - 4 * odd
    source = me - 2 + 4 * odd
    reach = max(distance for _, distance, _ in plan)

    in_copies = [
        pltpu.make_async_copy(source, into, in_sem.at[at])
        for at, (source, into) in enumerate((
            (third_hbm, third_ref), (second_hbm, second_ref), (fine_hbm, fine_ref),
            (bias_hbm, bias_ref), (proj_bias_hbm, proj_bias_ref)))
    ]
    for copy in in_copies:
        copy.start()
    weight_copies = {
        k: pltpu.make_async_copy(conv_hbm.at[k], weights.at[k], weight_sem.at[k])
        for k in WEIGHT_ORDER
    }
    proj_copy = pltpu.make_async_copy(proj_hbm, projs, proj_sem)
    for at, k in enumerate(WEIGHT_ORDER):
        weight_copies[k].start()
        if at == 2:
            proj_copy.start()

    barrier = pltpu.get_barrier_semaphore()
    for distance in range(1, reach + 1):
        @pl.when(me >= distance)
        def _():
            pl.semaphore_signal(barrier, inc=1, device_id={"rows": me - distance}, device_id_type=MESH)

        @pl.when(me + distance < devices)
        def _():
            pl.semaphore_signal(barrier, inc=1, device_id={"rows": me + distance}, device_id_type=MESH)
    expected = jnp.minimum(me, reach) + jnp.minimum(devices - 1 - me, reach)
    pl.semaphore_wait(barrier, expected)
    for copy in in_copies:
        copy.wait()

    up_copies, down_copies = [], []
    for at, (level, distance, rows) in enumerate(plan):
        block, halo = blocks[level], HALOS[level]
        up_at = halo - (distance - 1) * block - rows
        down_at = (distance - 1) * block
        up_copies.append(pltpu.make_async_remote_copy(
            src_ref=own[level].at[pl.ds(block - rows, rows)],
            dst_ref=ups[level].at[pl.ds(up_at, rows)],
            send_sem=up_send.at[at], recv_sem=up_recv.at[at],
            device_id={"rows": me + distance}, device_id_type=MESH))
        down_copies.append(pltpu.make_async_remote_copy(
            src_ref=own[level].at[pl.ds(0, rows)],
            dst_ref=downs[level].at[pl.ds(down_at, rows)],
            send_sem=down_send.at[at], recv_sem=down_recv.at[at],
            device_id={"rows": me - distance}, device_id_type=MESH))
        if level == THIRD:
            pl.when(me + distance < devices)(up_copies[at].start)
            pl.when(me >= distance)(down_copies[at].start)

    pair_copies, far_copies = {FINE: [], SECOND: []}, {FINE: [], SECOND: []}
    serial = 0
    for level in (SECOND, FINE):
        block = blocks[level]
        near = min(block, HALOS[level])
        for even_at, odd_at, rows, forwarded in pair_chunks(level, block):
            at = even_at + odd * (odd_at - even_at)
            pair_copies[level].append(pltpu.make_async_remote_copy(
                src_ref=own[level].at[pl.ds(at, rows)], dst_ref=peers[level].at[pl.ds(at, rows)],
                send_sem=pair_send.at[serial], recv_sem=pair_recv.at[serial],
                device_id={"rows": partner}, device_id_type=MESH))
            if forwarded:
                held = odd_at + odd * (even_at - odd_at)
                spot = held - (1 - odd) * (block - near)
                far_copies[level].append(pltpu.make_async_remote_copy(
                    src_ref=peers[level].at[pl.ds(held, rows)], dst_ref=fars[level].at[pl.ds(spot, rows)],
                    send_sem=far_send.at[serial], recv_sem=far_recv.at[serial],
                    device_id={"rows": target}, device_id_type=MESH))
            serial += 1
            pair_copies[level][-1].start()
        for at, (wanted, distance, _) in enumerate(plan):
            if wanted == level:
                pl.when(me + distance < devices)(up_copies[at].start)
                pl.when(me >= distance)(down_copies[at].start)
    has_target = jnp.logical_and(target >= 0, target < devices)
    has_source = jnp.logical_and(source >= 0, source < devices)

    def pass_on(level, chunk):
        pair_copies[level][chunk].wait_recv()
        if chunk < len(far_copies[level]):
            pl.when(has_target)(far_copies[level][chunk].start)

    def arrive(wanted):
        for at, (level, distance, _) in enumerate(plan):
            if level == wanted:
                pl.when(me >= distance)(up_copies[at].wait_recv)
                pl.when(me + distance < devices)(down_copies[at].wait_recv)
        for copy in far_copies.get(wanted, ()):
            pl.when(has_source)(copy.wait_recv)

    def inside(level, row):
        block = blocks[level]
        if 0 <= row < block:
            return None
        place = me * block + row
        return jnp.logical_and(place >= 0, place < devices * block)

    def store_padded(ref, at, values, level, first_row):
        steps = values.shape[1]
        for r in range(values.shape[0]):
            row = values[r:r + 1].astype(jnp.float32)
            valid = inside(level, first_row + r)
            if valid is not None:
                row = jnp.where(valid, row, 0.0)
            before, after = edge_steps(row, False)
            ref[at + r, 1:steps + 1] = row[0].astype(jnp.bfloat16)
            ref[at + r, 0] = before[0].astype(jnp.bfloat16)
            ref[at + r, steps + 1] = after[0].astype(jnp.bfloat16)

    def conv(ref, k, first, last, emit):
        steps = ref.shape[1] - 2
        tile = max(1, 512 // (steps * LANES))
        for r in range(first, last, tile):
            rows = min(tile, last - r)
            flat = jnp.concatenate(
                [ref[r + a:r + a + rows, b:b + steps].reshape(rows * steps * LANES, -1)
                 for a in range(3) for b in range(3)], axis=1)
            acc = jnp.dot(flat, weights[k], preferred_element_type=jnp.float32)
            acc = acc + bias_ref[k:k + 1, :]
            emit(r, acc.reshape(rows, steps, LANES, -1))

    def raw_row(level, place):
        block, halo = blocks[level], HALOS[level]
        near = min(block, halo)
        if 0 <= place < block:
            return own[level][place]
        if place < 0:
            j = -1 - place
            row = ups[level][halo - 1 - j] if level == THIRD or j >= block else None
            if row is None:
                row = jnp.where(even, fars[level][near - 1 - j], peers[level][block - 1 - j])
            return row
        j = place - block
        if level == THIRD or j >= block:
            return downs[level][j]
        return jnp.where(even, peers[level][j], fars[level][j])

    def take_rows(level, padded, first, last):
        halo = HALOS[level]
        columns = own[level].shape[1]
        steps = columns // LANES
        width = stage.shape[3]
        for place in range(first, last):
            row = raw_row(level, place).astype(jnp.float32)
            slot = place % stage.shape[0]
            parts = range(row.shape[1] // width)
            for c in parts:
                stage[slot, c, 0:columns] = row[:, c * width:(c + 1) * width]
            turned = jnp.concatenate(
                [jnp.concatenate([stage[slot, c, pl.ds(t, LANES, stride=steps), :] for c in parts], axis=1)[None]
                 for t in range(steps)], axis=0)
            fields[level][halo + place] = turned.astype(jnp.bfloat16)
            store_padded(padded, halo + place, jnp.maximum(turned, 0.0)[None], level, place)

    def hidden(level, source, target, k, first, last, row0):
        def emit(r, acc):
            store_padded(target, r, jnp.maximum(acc, 0.0), level, row0 + r)
        conv(source, k, first, last, emit)

    def source_rows(level, row, rows):
        at = HALOS[level] + row
        return fields[level][at:at + rows].astype(jnp.float32)

    def lift(level, refined, halo, index, emit, extra):
        count, steps = refined.shape[0], refined.shape[1]
        block = blocks[level]
        w = projs[index]
        tile = max(1, 512 // (steps * LANES))
        for r in range(0, count, tile):
            rows = min(tile, count - r)
            y = jnp.dot(refined[r:r + rows].reshape(rows * steps * LANES, -1), w,
                        preferred_element_type=jnp.float32)
            proj_y[r:r + rows, 0:steps] = y.reshape(rows, steps, LANES, -1)

        def line(m):
            value = proj_y[m, 0:steps]
            before, after = halo - 1 - m, m - halo - block
            if before >= 0 and before % block == 0:
                value = jnp.where(me == before // block, proj_y[m + 1, 0:steps], value)
            if after >= 0 and after % block == 0:
                value = jnp.where(me == devices - 1 - after // block, proj_y[m - 1, 0:steps], value)
            return value

        bias = proj_bias_ref[index:index + 1, :]

        def columns(out_row, major, minor):
            row = (0.75 * major + 0.25 * minor + bias)[None]
            before, after = edge_steps(row, True)
            wide = jnp.concatenate([before[:, None], row, after[:, None]], axis=1)[0]
            low = 0.25 * wide[0:steps] + 0.75 * row[0]
            high = 0.75 * row[0] + 0.25 * wide[2:steps + 2]
            emit(out_row, low.astype(jnp.bfloat16), high.astype(jnp.bfloat16))

        for m in range(count):
            even = 2 * (m - halo)
            if 1 <= m and (m < count - 1 or extra):
                columns(even, line(m), line(m - 1))
            if m < count - 1 and (m >= 1 or extra):
                columns(even + 1, line(m), line(m + 1))

    def emit_to(ref, first):
        def emit(row, low, high):
            for t in range(low.shape[0]):
                ref[row - first, 2 * t] = low[t]
                ref[row - first, 2 * t + 1] = high[t]
        return emit

    fill_table(table, own[FINE].shape[1])
    halo_f, halo_s, halo_t = HALOS
    block_f, block_s, block_t = blocks
    take_rows(FINE, padded_f, 0, block_f)
    weight_copies[6].wait()
    hidden(FINE, padded_f, hidden_f, 6, halo_f, halo_f + block_f - 2, 1 - halo_f)

    take_rows(THIRD, padded_t, 0, block_t)
    take_rows(SECOND, padded_s, 0, block_s)
    arrive(THIRD)
    take_rows(THIRD, padded_t, -halo_t, 0)
    take_rows(THIRD, padded_t, block_t, block_t + halo_t)
    pass_on(SECOND, 0)
    weight_copies[0].wait()
    hidden(THIRD, padded_t, hidden_t, 0, 0, block_t + 2 * halo_t - 2, 1 - halo_t)
    weight_copies[1].wait()

    def emit_third(r, acc):
        rows = acc.shape[0]
        total = acc + source_rows(THIRD, r + 2 - halo_t, rows)
        refined_t[r:r + rows] = total.astype(jnp.bfloat16)

    conv(hidden_t, 1, 0, block_t + 2 * halo_t - 4, emit_third)
    proj_copy.wait()
    lift(THIRD, refined_t, halo_t - 2, 0, emit_to(path_s, 2 - halo_s), False)

    def join(level, halo, padded, hidden_ref, merged, path, refined, k, early):
        block = blocks[level]
        last = block + 2 * halo
        if early:
            hidden(level, padded, hidden_ref, k, 0, early[0], 1 - halo)
            hidden(level, padded, hidden_ref, k, early[1], last - 2, 1 - halo)
        else:
            weight_copies[k].wait()
            hidden(level, padded, hidden_ref, k, 0, last - 2, 1 - halo)
        weight_copies[k + 1].wait()

        def emit_merged(r, acc):
            rows = acc.shape[0]
            total = acc + source_rows(level, r + 2 - halo, rows) + path[r:r + rows].astype(jnp.float32)
            total = total.astype(jnp.bfloat16)
            merged[r:r + rows] = total
            store_padded(padded, r, jnp.maximum(total, 0), level, r + 2 - halo)

        conv(hidden_ref, k + 1, 0, last - 4, emit_merged)
        if level == SECOND:
            pass_on(FINE, 1)
        weight_copies[k + 2].wait()
        hidden(level, padded, hidden_ref, k + 2, 0, last - 6, 3 - halo)
        weight_copies[k + 3].wait()

        def emit_refined(r, acc):
            rows = acc.shape[0]
            total = acc + merged[r + 2:r + 2 + rows].astype(jnp.float32)
            refined[r:r + rows] = total.astype(jnp.bfloat16)

        conv(hidden_ref, k + 3, 0, last - 8, emit_refined)

    pass_on(FINE, 0)
    arrive(SECOND)
    take_rows(SECOND, padded_s, -halo_s, 0)
    take_rows(SECOND, padded_s, block_s, block_s + halo_s)
    join(SECOND, halo_s, padded_s, hidden_s, merged_s, path_s, refined_s, 2, None)
    lift(SECOND, refined_s, halo_s - 4, 1, emit_to(path_f, 2 - halo_f), True)

    pass_on(FINE, 2)
    arrive(FINE)
    take_rows(FINE, padded_f, -halo_f, 0)
    take_rows(FINE, padded_f, block_f, block_f + halo_f)
    join(FINE, halo_f, padded_f, hidden_f, merged_f, path_f, refined_f, 6,
         (halo_f, halo_f + block_f - 2))
    count, steps_f = refined_f.shape[0], refined_f.shape[1]
    last_bias = proj_bias_ref[projs.shape[0] - 1:projs.shape[0], :]
    for r in range(0, count, count // 2):
        rows = count // 2
        y = jnp.dot(refined_f[r:r + rows].reshape(rows * steps_f * LANES, -1), projs[projs.shape[0] - 1],
                    preferred_element_type=jnp.float32) + last_bias
        lines_f[r:r + rows] = y.astype(jnp.bfloat16).reshape(rows, steps_f, LANES, -1)
    lines_f[0] = jnp.where(me == 0, lines_f[1].astype(jnp.float32), lines_f[0].astype(jnp.float32)).astype(jnp.bfloat16)
    lines_f[count - 1] = jnp.where(
        me == devices - 1, lines_f[count - 2].astype(jnp.float32),
        lines_f[count - 1].astype(jnp.float32)).astype(jnp.bfloat16)

    for at, (_, distance, _) in enumerate(plan):
        pl.when(me + distance < devices)(up_copies[at].wait_send)
        pl.when(me >= distance)(down_copies[at].wait_send)
    for level in (SECOND, FINE):
        for copy in pair_copies[level]:
            copy.wait_send()
        for copy in far_copies[level]:
            pl.when(has_target)(copy.wait_send)


def fill_table(table, columns):
    steps = columns // LANES
    wide = 2 * columns
    for half in range(2):
        for side in range(2):
            out = lax.broadcasted_iota(jnp.int32, (wide, columns), 0)
            place = lax.broadcasted_iota(jnp.int32, (wide, columns), 1)
            column = (place % LANES) * steps + place // LANES
            near = out // 2
            far = jnp.clip(near + 2 * (out % 2) - 1, 0, columns - 1)
            weight = jnp.where(column == near, 0.75, 0.0) + jnp.where(column == far, 0.25, 0.0)
            weight = weight * (0.75 if half == side else 0.25)
            table[half * wide:(half + 1) * wide, side * columns:(side + 1) * columns] = weight.astype(jnp.bfloat16)


def lift_kernel(lines_ref, table_ref, out_ref):
    at = pl.program_id(0)
    steps, channels = lines_ref.shape[1], lines_ref.shape[3]
    columns = steps * LANES
    wide = 2 * columns
    per = out_ref.shape[0] // 2
    for i in range(per + 1):
        pair = lines_ref[pl.ds(at * per + i, 2)].reshape(2 * columns, channels)
        first, last = (wide if i == 0 else 0), (wide if i == per else 2 * wide)
        rows = jnp.dot(table_ref[first:last], pair, preferred_element_type=jnp.float32).astype(jnp.bfloat16)
        if i > 0:
            out_ref[2 * i - 1] = rows[0:wide]
        if i < per:
            out_ref[2 * i] = rows[last - first - wide:]


def local(devices, feat_fine, feat_second, feat_third, conv_weight, conv_bias, out_weight, out_bias):
    fields = (feat_fine, feat_second, feat_third)
    channels = feat_fine.shape[2]
    blocks = [v.shape[0] for v in fields]
    columns = [v.shape[1] for v in fields]
    steps = [c // LANES for c in columns]
    width = min(128, channels)

    def raw(count, level):
        return pltpu.VMEM((count, columns[level], channels), jnp.bfloat16)

    def rows_of(count, level, extra=0, dtype=jnp.bfloat16):
        return pltpu.VMEM((count, steps[level] + extra, LANES, channels), dtype)

    extents = [block + 2 * halo for block, halo in zip(blocks, HALOS)]
    copies = len(direct_sends(blocks))
    pairs = sum(len(pair_chunks(level, blocks[level])) for level in (FINE, SECOND))
    dma = pltpu.SemaphoreType.DMA
    scratch = [raw(blocks[level], level) for level in range(3)]
    scratch += [pltpu.VMEM(conv_bias.shape, jnp.float32), pltpu.VMEM(out_bias.shape, jnp.float32)]
    scratch += [raw(HALOS[level], level) for level in range(3) for _ in range(2)]
    for level in (FINE, SECOND):
        scratch += [raw(blocks[level], level), raw(min(blocks[level], HALOS[level]), level)]
    scratch += [rows_of(extents[level], level) for level in range(3)]
    scratch += [pltpu.VMEM((8, channels // width, columns[FINE], width), jnp.float32)]
    scratch += [pltpu.VMEM((conv_weight.shape[0], 9 * channels, channels), jnp.bfloat16),
                pltpu.VMEM(out_weight.shape, jnp.bfloat16)]
    for level in (FINE, SECOND):
        scratch += [rows_of(extents[level], level, 2), rows_of(extents[level] - 2, level, 2),
                    rows_of(extents[level] - 4, level), rows_of(extents[level] - 4, level)]
    scratch += [rows_of(extents[THIRD], THIRD, 2), rows_of(extents[THIRD] - 2, THIRD, 2)]
    scratch += [rows_of(extents[FINE] - 8, FINE), rows_of(extents[SECOND] - 8, SECOND),
                rows_of(extents[THIRD] - 4, THIRD)]
    scratch += [rows_of(max(extents[SECOND] - 8, extents[THIRD] - 4), SECOND, 0, jnp.float32)]
    scratch += [dma((copies,)) for _ in range(4)] + [dma((pairs,)) for _ in range(4)] + [dma((conv_weight.shape[0],)), dma, dma((5,))]
    vmem, far = pl.BlockSpec(memory_space=pltpu.VMEM), pl.BlockSpec(memory_space=pltpu.HBM)
    wide = 2 * columns[FINE]
    lines, table = pl.pallas_call(
        functools.partial(kernel, devices),
        out_shape=[jax.ShapeDtypeStruct((extents[FINE] - 8, steps[FINE], LANES, channels), jnp.bfloat16),
                   jax.ShapeDtypeStruct((2 * wide, 2 * columns[FINE]), jnp.bfloat16)],
        in_specs=[far] * 7,
        out_specs=[vmem, vmem],
        scratch_shapes=scratch,
        compiler_params=pltpu.CompilerParams(
            collective_id=0, has_side_effects=True, vmem_limit_bytes=VMEM_MIB * 1024 * 1024),
    )(*[pltpu.with_memory_space_constraint(v, pltpu.HBM) for v in (
        *fields, conv_weight.reshape(conv_weight.shape[0], 9 * channels, channels), conv_bias, out_weight, out_bias)])
    per = 2 if blocks[FINE] % 2 == 0 else 1
    return pl.pallas_call(
        lift_kernel,
        grid=(blocks[FINE] // per,),
        out_shape=jax.ShapeDtypeStruct((2 * blocks[FINE], wide, channels), jnp.bfloat16),
        in_specs=[vmem, vmem],
        out_specs=pl.BlockSpec((2 * per, wide, channels), lambda g: (g, 0, 0)),
        compiler_params=pltpu.CompilerParams(vmem_limit_bytes=8 * 1024 * 1024),
    )(lines, table)


def solution(mesh):
    rows = P(("img", "rows"), None, None)
    return jax.shard_map(
        functools.partial(local, mesh.shape["rows"]),
        mesh=mesh,
        in_specs=(rows, rows, rows, P(), P(), P(), P()),
        out_specs=rows,
        check_vma=False,
    )
```

```python
import functools

import jax
import jax.numpy as jnp
from jax import lax
from jax.experimental import pallas as pl
from jax.experimental.pallas import tpu as pltpu
from jax.sharding import PartitionSpec as P

MESH = pl.DeviceIdType.MESH
LANES = 16
VMEM_MIB = 44
MOST = 640
RING = 2
FINE, SECOND, THIRD = 0, 1, 2
HALOS = (5, 6, 5)
WEIGHT_ORDER = (6, 7, 2, 0, 1, 3, 4, 5, 8, 9)


def direct_rows(level, block):
    halo = HALOS[level]
    return [(d, min(block, halo - (d - 1) * block)) for d in range(2, -(-halo // block) + 1)]


def pair_rows(level, block):
    near = min(block, HALOS[level])
    if level == THIRD:
        return [(0, block, True)]
    if level == SECOND:
        cuts = [block, block // 2, 0] if block > 1 else [block, 0]
        return [(low, high - low, True) for high, low in zip(cuts, cuts[1:])]
    away, beside = list(range(block - 1, -1, -1)), list(range(block))
    order = away[:RING] + beside[:RING] + away[RING:near]
    order = list(dict.fromkeys(order + beside[:near] + away))
    return [(r, 1, r >= block - near) for r in order]


def pairs_of(first, last, most):
    rows = last - first
    parts = min(rows, 2 * -(-rows // (2 * most)))
    cuts = [first + rows * i // parts for i in range(parts + 1)]
    return [(p, q - p) for p, q in zip(cuts, cuts[1:])]


def edge_steps(values, clamp):
    steps = values.shape[1]
    first, last = values[:, 0], values[:, steps - 1]
    place = lax.broadcasted_iota(jnp.int32, first.shape, 1)
    zero = jnp.zeros_like(first)
    before = jnp.where(place == 0, first if clamp else zero, pltpu.roll(last, 1, 1))
    after = jnp.where(place == LANES - 1, last if clamp else zero, pltpu.roll(first, LANES - 1, 1))
    return before, after


def kernel(
    devices, fine_hbm, second_hbm, third_hbm, conv_hbm, bias_hbm, proj_hbm, proj_bias_hbm, lines_f, table,
    fine_ref, second_ref, third_ref, bias_ref, proj_bias_ref,
    fine_other, second_other, third_other,
    second_up, second_down, third_up, third_down,
    fine_x, second_x, third_x, stage, weights, projs,
    padded_f, hidden_f, addend_f, joined_f, hidden2_f, merged_f, path_f,
    padded_s, hidden_s, merged_s, path_s,
    padded_t, hidden_t, refined_f, refined_s, refined_t, proj_y,
    up_send, up_recv, down_send, down_recv, up2_send, down2_send,
    pair_send, pair_recv, far_send, far_recv, weight_sem, proj_sem, in_sem,
):
    me = lax.axis_index("rows")
    own = (fine_ref, second_ref, third_ref)
    ups = (None, second_up, third_up)
    downs = (None, second_down, third_down)
    blocks = tuple(ref.shape[0] for ref in own)
    fields = (fine_x, second_x, third_x)
    others = (fine_other, second_other, third_other)
    odd = me % 2
    even = odd == 0
    is_odd = odd == 1
    partner = me + 1 - 2 * odd
    target = me + 2 - 4 * odd
    source = me - 2 + 4 * odd

    in_copies = [
        pltpu.make_async_copy(source_ref, into, in_sem.at[at])
        for at, (source_ref, into) in enumerate((
            (second_hbm, second_ref), (third_hbm, third_ref), (fine_hbm, fine_ref),
            (bias_hbm, bias_ref), (proj_bias_hbm, proj_bias_ref)))
    ]
    for copy in in_copies:
        copy.start()
    weight_copies = {
        k: pltpu.make_async_copy(conv_hbm.at[k], weights.at[k], weight_sem.at[k])
        for k in WEIGHT_ORDER
    }
    proj_copy = pltpu.make_async_copy(proj_hbm, projs, proj_sem)
    for at, k in enumerate(WEIGHT_ORDER):
        weight_copies[k].start()
        if at == 3:
            proj_copy.start()

    reach = max([2] + [d for level in (SECOND, THIRD) for d, _ in direct_rows(level, blocks[level])])
    barrier = pltpu.get_barrier_semaphore()
    for distance in range(1, reach + 1):
        @pl.when(me >= distance)
        def _():
            pl.semaphore_signal(barrier, inc=1, device_id={"rows": me - distance}, device_id_type=MESH)

        @pl.when(me + distance < devices)
        def _():
            pl.semaphore_signal(barrier, inc=1, device_id={"rows": me + distance}, device_id_type=MESH)
    expected = jnp.minimum(me, reach) + jnp.minimum(devices - 1 - me, reach)
    pl.semaphore_wait(barrier, expected)
    for copy in in_copies:
        copy.wait()

    has_target = jnp.logical_and(target >= 0, target < devices)
    has_source = jnp.logical_and(source >= 0, source < devices)

    def remote(src, dst, send, recv, device):
        return pltpu.make_async_remote_copy(
            src_ref=src, dst_ref=dst, send_sem=send, recv_sem=recv,
            device_id={"rows": device}, device_id_type=MESH)

    starts, sends, arrivals, relays = [], [], {THIRD: [], SECOND: []}, {THIRD: [], SECOND: []}
    serial = 0
    for level in (THIRD, SECOND):
        block, halo = blocks[level], HALOS[level]
        for distance, rows in direct_rows(level, block):
            at = serial
            serial += 1
            up_src, up_dst = pl.ds(block - rows, rows), pl.ds(halo - (distance - 1) * block - rows, rows)
            down_src, down_dst = pl.ds(0, rows), pl.ds((distance - 1) * block, rows)
            up = remote(own[level].at[up_src], ups[level].at[up_dst], up_send.at[at], up_recv.at[at], me + distance)
            down = remote(
                own[level].at[down_src], downs[level].at[down_dst], down_send.at[at], down_recv.at[at], me - distance)
            up_ok, down_ok = me + distance < devices, me >= distance
            arrivals[level] += [(down_ok, up), (up_ok, down)]
            if distance % 2 == 0:
                starts += [(level, up_ok, up), (level, down_ok, down)]
                sends += [(up_ok, up), (down_ok, down)]
                continue
            up_ok, down_ok = jnp.logical_and(is_odd, up_ok), jnp.logical_and(even, down_ok)
            starts += [(level, up_ok, up), (level, down_ok, down)]
            sends += [(up_ok, up), (down_ok, down)]
            hop = distance - 1
            up2 = remote(
                others[level].at[up_src], ups[level].at[up_dst], up2_send.at[at], up_recv.at[at], me + hop)
            down2 = remote(
                others[level].at[down_src], downs[level].at[down_dst], down2_send.at[at], down_recv.at[at], me - hop)
            up2_ok = jnp.logical_and(is_odd, me + hop < devices)
            down2_ok = jnp.logical_and(even, me >= hop)
            relays[level] += [(up2_ok, up2), (down2_ok, down2)]
            sends += [(up2_ok, up2), (down2_ok, down2)]

    pair_copies, far_copies = {}, {}
    serial = 0
    for level in (SECOND, THIRD, FINE):
        block = blocks[level]
        near = min(block, HALOS[level])
        pair_copies[level], far_copies[level] = [], []
        for row, rows, forwarded in pair_rows(level, block):
            mirrored = block - row - rows
            at = mirrored + odd * (row - mirrored)
            pair_copies[level].append(remote(
                own[level].at[pl.ds(at, rows)], others[level].at[pl.ds(at, rows)],
                pair_send.at[serial], pair_recv.at[serial], partner))
            relay = None
            if forwarded:
                held = row + odd * (mirrored - row)
                spot = block + held - (1 - odd) * (block - near)
                relay = remote(
                    others[level].at[pl.ds(held, rows)], others[level].at[pl.ds(spot, rows)],
                    far_send.at[serial], far_recv.at[serial], target)
            far_copies[level].append(relay)
            serial += 1
        for wanted, ok, copy in starts:
            if wanted == level:
                pl.when(ok)(copy.start)
        for copy in pair_copies[level]:
            copy.start()

    def pass_on(level, chunk):
        pair_copies[level][chunk].wait_recv()
        if far_copies[level][chunk] is not None:
            pl.when(has_target)(far_copies[level][chunk].start)
        for ok, copy in relays.get(level, ()):
            pl.when(ok)(copy.start)

    def arrive(level):
        for ok, copy in arrivals[level]:
            pl.when(ok)(copy.wait_recv)
        for copy in far_copies[level]:
            pl.when(has_source)(copy.wait_recv)

    def inside(level, row):
        block = blocks[level]
        if 0 <= row < block:
            return None
        place = me * block + row
        return jnp.logical_and(place >= 0, place < devices * block)

    def store_padded(ref, at, values, level, first_row):
        steps = values.shape[1]
        for r in range(values.shape[0]):
            row = values[r:r + 1].astype(jnp.float32)
            valid = inside(level, first_row + r)
            if valid is not None:
                row = jnp.where(valid, row, 0.0)
            before, after = edge_steps(row, False)
            ref[at + r, 1:steps + 1] = row[0].astype(jnp.bfloat16)
            ref[at + r, 0] = before[0].astype(jnp.bfloat16)
            ref[at + r, steps + 1] = after[0].astype(jnp.bfloat16)

    def conv(ref, k, tiles, emit):
        steps = ref.shape[1] - 2
        for r, rows in tiles:
            flat = jnp.concatenate(
                [ref[r + a:r + a + rows, b:b + steps].reshape(rows * steps * LANES, -1)
                 for a in range(3) for b in range(3)], axis=1)
            acc = jnp.dot(flat, weights[k], preferred_element_type=jnp.float32)
            acc = acc + bias_ref[k:k + 1, :]
            emit(r, acc.reshape(rows, steps, LANES, -1))

    def tiles_of(level, first, last):
        return pairs_of(first, last, max(1, MOST // own[level].shape[1]))

    def raw_row(level, place):
        block, halo = blocks[level], HALOS[level]
        near = min(block, halo)
        if 0 <= place < block:
            return own[level][place]
        if place < 0:
            j = -1 - place
            if j >= block:
                return ups[level][halo - 1 - j]
            return others[level][block - 1 - j + (1 - odd) * near]
        j = place - block
        if j >= block:
            return downs[level][j]
        return others[level][j + odd * block]

    def take_rows(level, padded, first, last):
        halo = HALOS[level]
        columns = own[level].shape[1]
        steps = columns // LANES
        width = stage.shape[3]
        for place in range(first, last):
            row = raw_row(level, place).astype(jnp.float32)
            slot = place % stage.shape[0]
            parts = range(row.shape[1] // width)
            for c in parts:
                stage[slot, c, 0:columns] = row[:, c * width:(c + 1) * width]
            turned = jnp.concatenate(
                [jnp.concatenate([stage[slot, c, pl.ds(t, LANES, stride=steps), :] for c in parts], axis=1)[None]
                 for t in range(steps)], axis=0)
            fields[level][halo + place] = turned.astype(jnp.bfloat16)
            store_padded(padded, halo + place, jnp.maximum(turned, 0.0)[None], level, place)

    def hidden(level, source, target, k, tiles, row0):
        def emit(r, acc):
            store_padded(target, r, jnp.maximum(acc, 0.0), level, row0 + r)
        conv(source, k, tiles, emit)

    def source_rows(level, row, rows):
        at = HALOS[level] + row
        return fields[level][at:at + rows].astype(jnp.float32)

    def lift(level, refined, halo, index, emit, extra):
        count, steps = refined.shape[0], refined.shape[1]
        block = blocks[level]
        w = projs[index]
        tile = max(1, 512 // (steps * LANES))
        for r in range(0, count, tile):
            rows = min(tile, count - r)
            y = jnp.dot(refined[r:r + rows].reshape(rows * steps * LANES, -1), w,
                        preferred_element_type=jnp.float32)
            proj_y[r:r + rows, 0:steps] = y.reshape(rows, steps, LANES, -1)

        def line(m):
            value = proj_y[m, 0:steps]
            before, after = halo - 1 - m, m - halo - block
            if before >= 0 and before % block == 0:
                value = jnp.where(me == before // block, proj_y[m + 1, 0:steps], value)
            if after >= 0 and after % block == 0:
                value = jnp.where(me == devices - 1 - after // block, proj_y[m - 1, 0:steps], value)
            return value

        bias = proj_bias_ref[index:index + 1, :]

        def columns(out_row, major, minor):
            row = (0.75 * major + 0.25 * minor + bias)[None]
            before, after = edge_steps(row, True)
            wide = jnp.concatenate([before[:, None], row, after[:, None]], axis=1)[0]
            low = 0.25 * wide[0:steps] + 0.75 * row[0]
            high = 0.75 * row[0] + 0.25 * wide[2:steps + 2]
            emit(out_row, low.astype(jnp.bfloat16), high.astype(jnp.bfloat16))

        for m in range(count):
            even = 2 * (m - halo)
            if 1 <= m and (m < count - 1 or extra):
                columns(even, line(m), line(m - 1))
            if m < count - 1 and (m >= 1 or extra):
                columns(even + 1, line(m), line(m + 1))

    def emit_to(ref, first):
        def emit(row, low, high):
            for t in range(low.shape[0]):
                ref[row - first, 2 * t] = low[t]
                ref[row - first, 2 * t + 1] = high[t]
        return emit

    halo_f, halo_s, halo_t = HALOS
    block_f, block_s, block_t = blocks
    order = [row for row, _, _ in pair_rows(FINE, block_f)]

    def fine_unit(tiles):
        def emit(r, acc):
            rows = acc.shape[0]
            addend_f[r:r + rows] = acc + source_rows(FINE, r + 2 - halo_f, rows)
        conv(hidden_f, 7, tiles, emit)

    def fine_join(first, last):
        for r in range(first, last):
            total = (addend_f[r:r + 1] + path_f[r:r + 1].astype(jnp.float32)).astype(jnp.bfloat16)
            merged_f[r:r + 1] = total
            store_padded(joined_f, r, jnp.maximum(total, 0), FINE, r + 2 - halo_f)

    def fine_refined(tiles):
        def emit(r, acc):
            rows = acc.shape[0]
            refined_f[r:r + rows] = (acc + merged_f[r + 2:r + 2 + rows].astype(jnp.float32)).astype(jnp.bfloat16)
        conv(hidden2_f, 9, tiles, emit)

    last_index = projs.shape[0] - 1

    def project(tiles):
        bias = proj_bias_ref[last_index:last_index + 1, :]
        for r, rows in tiles:
            y = jnp.dot(refined_f[r:r + rows].reshape(rows * refined_f.shape[1] * LANES, -1), projs[last_index],
                        preferred_element_type=jnp.float32) + bias
            lines_f[r:r + rows] = y.astype(jnp.bfloat16).reshape(rows, refined_f.shape[1], LANES, -1)

    take_rows(FINE, padded_f, 0, block_f)
    weight_copies[6].wait()
    hidden(FINE, padded_f, hidden_f, 6, tiles_of(FINE, halo_f, halo_f + block_f - 2), 1 - halo_f)
    weight_copies[7].wait()
    fine_unit(tiles_of(FINE, halo_f, halo_f + block_f - 4))
    for at in range(len(pair_copies[SECOND])):
        pass_on(SECOND, at)
    take_rows(THIRD, padded_t, 0, block_t)
    take_rows(SECOND, padded_s, 0, block_s)
    fill_table(table, own[FINE].shape[1])
    pass_on(THIRD, 0)

    last_s = block_s + 2 * halo_s
    arrive(SECOND)
    pass_on(FINE, 0)
    take_rows(SECOND, padded_s, -halo_s, 0)
    take_rows(SECOND, padded_s, block_s, block_s + halo_s)
    weight_copies[2].wait()
    hidden(SECOND, padded_s, hidden_s, 2, tiles_of(SECOND, 0, last_s - 2), 1 - halo_s)
    arrive(THIRD)
    pass_on(FINE, 1)
    take_rows(THIRD, padded_t, -halo_t, 0)
    take_rows(THIRD, padded_t, block_t, block_t + halo_t)
    weight_copies[0].wait()
    weight_copies[1].wait()
    weight_copies[3].wait()
    proj_copy.wait()
    hidden(THIRD, padded_t, hidden_t, 0, tiles_of(THIRD, 0, block_t + 2 * halo_t - 2), 1 - halo_t)

    def emit_third(r, acc):
        rows = acc.shape[0]
        total = acc + source_rows(THIRD, r + 2 - halo_t, rows)
        refined_t[r:r + rows] = total.astype(jnp.bfloat16)

    conv(hidden_t, 1, tiles_of(THIRD, 0, block_t + 2 * halo_t - 4), emit_third)
    lift(THIRD, refined_t, halo_t - 2, 0, emit_to(path_s, 2 - halo_s), False)

    def emit_merged(r, acc):
        rows = acc.shape[0]
        total = acc + source_rows(SECOND, r + 2 - halo_s, rows) + path_s[r:r + rows].astype(jnp.float32)
        total = total.astype(jnp.bfloat16)
        merged_s[r:r + rows] = total
        store_padded(padded_s, r, jnp.maximum(total, 0), SECOND, r + 2 - halo_s)

    conv(hidden_s, 3, tiles_of(SECOND, 0, last_s - 4), emit_merged)
    pass_on(FINE, 2)
    pass_on(FINE, 3)

    weight_copies[4].wait()
    weight_copies[5].wait()
    hidden(SECOND, padded_s, hidden_s, 4, tiles_of(SECOND, 0, last_s - 6), 3 - halo_s)

    def emit_refined(r, acc):
        rows = acc.shape[0]
        total = acc + merged_s[r + 2:r + 2 + rows].astype(jnp.float32)
        refined_s[r:r + rows] = total.astype(jnp.bfloat16)

    conv(hidden_s, 5, tiles_of(SECOND, 0, last_s - 8), emit_refined)
    pass_on(FINE, 4)

    ring = RING
    wide_f = block_f + 2 * halo_f
    far_of = {row: at for at, row in enumerate(order)}
    for d in range(ring):
        pl.when(has_source)(far_copies[FINE][far_of[block_f - 1 - d]].wait_recv)
    lift(SECOND, refined_s, halo_s - 4, 1, emit_to(path_f, 2 - halo_f), True)
    take_rows(FINE, padded_f, -ring, 0)
    take_rows(FINE, padded_f, block_f, block_f + ring)
    hidden(FINE, padded_f, hidden_f, 6, [(halo_f - ring, ring), (halo_f + block_f - 2, ring)], 1 - halo_f)
    fine_unit([(halo_f - ring, ring), (halo_f + block_f - 4, ring)])
    low, high = halo_f - 2, halo_f - 2 + block_f
    fine_join(low, high)
    pass_on(FINE, 5)
    weight_copies[8].wait()
    weight_copies[9].wait()
    hidden(FINE, joined_f, hidden2_f, 8, tiles_of(FINE, low, high - 2), 3 - halo_f)
    pass_on(FINE, 6)
    fine_refined(tiles_of(FINE, low, high - 4))
    project(tiles_of(FINE, low, high - 4))

    for at in range(7, len(order)):
        pass_on(FINE, at)
    for at, row in enumerate(order):
        if far_copies[FINE][at] is not None and row < block_f - ring:
            pl.when(has_source)(far_copies[FINE][at].wait_recv)
    take_rows(FINE, padded_f, -halo_f, -ring)
    take_rows(FINE, padded_f, block_f + ring, block_f + halo_f)
    edge = halo_f - ring
    ends = lambda count: [(0, edge), (count - edge, edge)]
    hidden(FINE, padded_f, hidden_f, 6, ends(wide_f - 2), 1 - halo_f)
    fine_unit(ends(wide_f - 4))
    fine_join(0, edge)
    fine_join(wide_f - 4 - edge, wide_f - 4)
    hidden(FINE, joined_f, hidden2_f, 8, ends(wide_f - 6), 3 - halo_f)
    fine_refined(ends(wide_f - 8))
    project(ends(wide_f - 8))
    count = lines_f.shape[0]
    for end, beside, at_end in ((0, 1, me == 0), (count - 1, count - 2, me == devices - 1)):
        lines_f[end] = jnp.where(
            at_end, lines_f[beside].astype(jnp.float32), lines_f[end].astype(jnp.float32)).astype(jnp.bfloat16)

    for ok, copy in sends:
        pl.when(ok)(copy.wait_send)
    for level in (THIRD, SECOND, FINE):
        for copy in pair_copies[level]:
            copy.wait_send()
        for copy in far_copies[level]:
            if copy is not None:
                pl.when(has_target)(copy.wait_send)


def fill_table(table, columns):
    steps = columns // LANES
    wide = 2 * columns
    for half in range(2):
        for side in range(2):
            out = lax.broadcasted_iota(jnp.int32, (wide, columns), 0)
            place = lax.broadcasted_iota(jnp.int32, (wide, columns), 1)
            column = (place % LANES) * steps + place // LANES
            near = out // 2
            far = jnp.clip(near + 2 * (out % 2) - 1, 0, columns - 1)
            weight = jnp.where(column == near, 0.75, 0.0) + jnp.where(column == far, 0.25, 0.0)
            weight = weight * (0.75 if half == side else 0.25)
            table[half * wide:(half + 1) * wide, side * columns:(side + 1) * columns] = weight.astype(jnp.bfloat16)


def lift_kernel(lines_ref, table_ref, out_ref):
    at = pl.program_id(0)
    steps, channels = lines_ref.shape[1], lines_ref.shape[3]
    columns = steps * LANES
    wide = 2 * columns
    per = out_ref.shape[0] // 2
    for i in range(per + 1):
        pair = lines_ref[pl.ds(at * per + i, 2)].reshape(2 * columns, channels)
        first, last = (wide if i == 0 else 0), (wide if i == per else 2 * wide)
        rows = jnp.dot(table_ref[first:last], pair, preferred_element_type=jnp.float32).astype(jnp.bfloat16)
        if i > 0:
            out_ref[2 * i - 1] = rows[0:wide]
        if i < per:
            out_ref[2 * i] = rows[last - first - wide:]


def local(devices, feat_fine, feat_second, feat_third, conv_weight, conv_bias, out_weight, out_bias):
    fields = (feat_fine, feat_second, feat_third)
    channels = feat_fine.shape[2]
    blocks = [v.shape[0] for v in fields]
    columns = [v.shape[1] for v in fields]
    steps = [c // LANES for c in columns]
    width = min(128, channels)

    def raw(count, level):
        return pltpu.VMEM((count, columns[level], channels), jnp.bfloat16)

    def rows_of(count, level, extra=0, dtype=jnp.bfloat16):
        return pltpu.VMEM((count, steps[level] + extra, LANES, channels), dtype)

    extents = [block + 2 * halo for block, halo in zip(blocks, HALOS)]
    copies = sum(len(direct_rows(level, blocks[level])) for level in (SECOND, THIRD))
    pairs = sum(len(pair_rows(level, blocks[level])) for level in range(3))
    dma = pltpu.SemaphoreType.DMA
    scratch = [raw(blocks[level], level) for level in range(3)]
    scratch += [pltpu.VMEM(conv_bias.shape, jnp.float32), pltpu.VMEM(out_bias.shape, jnp.float32)]
    for level in range(3):
        scratch += [raw(blocks[level] + min(blocks[level], HALOS[level]), level)]
    scratch += [raw(HALOS[level], level) for level in (SECOND, THIRD) for _ in range(2)]
    scratch += [rows_of(extents[level], level) for level in range(3)]
    scratch += [pltpu.VMEM((8, channels // width, columns[FINE], width), jnp.float32)]
    scratch += [pltpu.VMEM((conv_weight.shape[0], 9 * channels, channels), jnp.bfloat16),
                pltpu.VMEM(out_weight.shape, jnp.bfloat16)]
    scratch += [rows_of(extents[FINE], FINE, 2), rows_of(extents[FINE] - 2, FINE, 2),
                rows_of(extents[FINE] - 4, FINE, 0, jnp.float32), rows_of(extents[FINE] - 4, FINE, 2),
                rows_of(extents[FINE] - 6, FINE, 2), rows_of(extents[FINE] - 4, FINE), rows_of(extents[FINE] - 4, FINE)]
    scratch += [rows_of(extents[SECOND], SECOND, 2), rows_of(extents[SECOND] - 2, SECOND, 2),
                rows_of(extents[SECOND] - 4, SECOND), rows_of(extents[SECOND] - 4, SECOND)]
    scratch += [rows_of(extents[THIRD], THIRD, 2), rows_of(extents[THIRD] - 2, THIRD, 2)]
    scratch += [rows_of(extents[FINE] - 8, FINE), rows_of(extents[SECOND] - 8, SECOND),
                rows_of(extents[THIRD] - 4, THIRD)]
    scratch += [rows_of(max(extents[SECOND] - 8, extents[THIRD] - 4), SECOND, 0, jnp.float32)]
    scratch += [dma((copies,)) for _ in range(6)] + [dma((pairs,)) for _ in range(4)]
    scratch += [dma((conv_weight.shape[0],)), dma, dma((5,))]
    vmem, far = pl.BlockSpec(memory_space=pltpu.VMEM), pl.BlockSpec(memory_space=pltpu.HBM)
    wide = 2 * columns[FINE]
    lines, table = pl.pallas_call(
        functools.partial(kernel, devices),
        out_shape=[jax.ShapeDtypeStruct((extents[FINE] - 8, steps[FINE], LANES, channels), jnp.bfloat16),
                   jax.ShapeDtypeStruct((2 * wide, 2 * columns[FINE]), jnp.bfloat16)],
        in_specs=[far] * 7,
        out_specs=[vmem, vmem],
        scratch_shapes=scratch,
        compiler_params=pltpu.CompilerParams(
            collective_id=0, has_side_effects=True, vmem_limit_bytes=VMEM_MIB * 1024 * 1024),
    )(*[pltpu.with_memory_space_constraint(v, pltpu.HBM) for v in (
        *fields, conv_weight.reshape(conv_weight.shape[0], 9 * channels, channels), conv_bias, out_weight, out_bias)])
    per = 2 if blocks[FINE] % 2 == 0 else 1
    return pl.pallas_call(
        lift_kernel,
        grid=(blocks[FINE] // per,),
        out_shape=jax.ShapeDtypeStruct((2 * blocks[FINE], wide, channels), jnp.bfloat16),
        in_specs=[vmem, vmem],
        out_specs=pl.BlockSpec((2 * per, wide, channels), lambda g: (g, 0, 0)),
        compiler_params=pltpu.CompilerParams(vmem_limit_bytes=8 * 1024 * 1024),
    )(lines, table)


def solution(mesh):
    rows = P(("img", "rows"), None, None)
    return jax.shard_map(
        functools.partial(local, mesh.shape["rows"]),
        mesh=mesh,
        in_specs=(rows, rows, rows, P(), P(), P(), P()),
        out_specs=rows,
        check_vma=False,
    )
```

```python
import functools

import jax
import jax.numpy as jnp
from jax import lax
from jax.experimental import pallas as pl
from jax.experimental.pallas import tpu as pltpu
from jax.sharding import PartitionSpec as P

MESH = pl.DeviceIdType.MESH
LANES = 16
VMEM_MIB = 52
MOST = 640
RING = 1
FINE, SECOND, THIRD = 0, 1, 2
HALOS = (5, 6, 5)
WEIGHT_ORDER = (6, 7, 2, 0, 1, 3, 4, 5, 8, 9)


def direct_rows(level, block):
    halo = HALOS[level]
    return [(d, min(block, halo - (d - 1) * block)) for d in range(2, -(-halo // block) + 1)]


def pair_rows(level, block):
    near = min(block, HALOS[level])
    if level == THIRD:
        return [(0, block, True)]
    if level == SECOND:
        cuts = [block, block // 2, 0] if block > 1 else [block, 0]
        return [(low, high - low, True) for high, low in zip(cuts, cuts[1:])]
    away, beside = list(range(block - 1, -1, -1)), list(range(block))
    order = away[:2] + beside[:RING] + away[2:near]
    order = list(dict.fromkeys(order + beside[:near] + away))
    return [(r, 1, r >= block - near) for r in order]


def parts_of(first, last, most):
    rows = last - first
    parts = -(-rows // most)
    cuts = [first + rows * i // parts for i in range(parts + 1)]
    return [(p, q - p) for p, q in zip(cuts, cuts[1:])]


def edge_steps(values, clamp):
    steps = values.shape[1]
    first, last = values[:, 0], values[:, steps - 1]
    place = lax.broadcasted_iota(jnp.int32, first.shape, 1)
    zero = jnp.zeros_like(first)
    before = jnp.where(place == 0, first if clamp else zero, pltpu.roll(last, 1, 1))
    after = jnp.where(place == LANES - 1, last if clamp else zero, pltpu.roll(first, LANES - 1, 1))
    return before, after


def kernel(
    devices, fine_hbm, second_hbm, third_hbm, conv_hbm, bias_hbm, proj_hbm, proj_bias_hbm, lines_f, table,
    fine_ref, second_ref, third_ref, bias_ref, proj_bias_ref,
    fine_other, second_other, third_other,
    second_up, second_down, third_up, third_down,
    fine_x, second_x, third_x, stage, weights, mixed, projs,
    padded_f, hidden_f, addend_f, joined_f, hidden2_f, merged_f, path_f,
    padded_s, hidden_s, merged_s, path_s,
    padded_t, hidden_t, refined_f, refined_s, refined_t, proj_y,
    up_send, up_recv, down_send, down_recv, up2_send, down2_send,
    pair_send, pair_recv, far_send, far_recv, weight_sem, proj_sem, in_sem,
):
    me = lax.axis_index("rows")
    own = (fine_ref, second_ref, third_ref)
    ups = (None, second_up, third_up)
    downs = (None, second_down, third_down)
    blocks = tuple(ref.shape[0] for ref in own)
    fields = (fine_x, second_x, third_x)
    others = (fine_other, second_other, third_other)
    odd = me % 2
    even = odd == 0
    is_odd = odd == 1
    partner = me + 1 - 2 * odd
    target = me + 2 - 4 * odd
    source = me - 2 + 4 * odd

    in_copies = [
        pltpu.make_async_copy(source_ref, into, in_sem.at[at])
        for at, (source_ref, into) in enumerate((
            (second_hbm, second_ref), (third_hbm, third_ref), (fine_hbm, fine_ref),
            (bias_hbm, bias_ref), (proj_bias_hbm, proj_bias_ref)))
    ]
    for copy in in_copies:
        copy.start()
    weight_copies = {
        k: pltpu.make_async_copy(conv_hbm.at[k], weights.at[k], weight_sem.at[k])
        for k in WEIGHT_ORDER
    }
    proj_copy = pltpu.make_async_copy(proj_hbm, projs, proj_sem)
    for at, k in enumerate(WEIGHT_ORDER):
        weight_copies[k].start()
        if at == 3:
            proj_copy.start()

    reach = max([2] + [d for level in (SECOND, THIRD) for d, _ in direct_rows(level, blocks[level])])
    barrier = pltpu.get_barrier_semaphore()
    for distance in range(1, reach + 1):
        @pl.when(me >= distance)
        def _():
            pl.semaphore_signal(barrier, inc=1, device_id={"rows": me - distance}, device_id_type=MESH)

        @pl.when(me + distance < devices)
        def _():
            pl.semaphore_signal(barrier, inc=1, device_id={"rows": me + distance}, device_id_type=MESH)
    expected = jnp.minimum(me, reach) + jnp.minimum(devices - 1 - me, reach)
    pl.semaphore_wait(barrier, expected)
    for copy in in_copies:
        copy.wait()

    has_target = jnp.logical_and(target >= 0, target < devices)
    has_source = jnp.logical_and(source >= 0, source < devices)

    def remote(src, dst, send, recv, device):
        return pltpu.make_async_remote_copy(
            src_ref=src, dst_ref=dst, send_sem=send, recv_sem=recv,
            device_id={"rows": device}, device_id_type=MESH)

    starts, sends, arrivals, relays = [], [], {THIRD: [], SECOND: []}, {THIRD: [], SECOND: []}
    serial = 0
    for level in (THIRD, SECOND):
        block, halo = blocks[level], HALOS[level]
        for distance, rows in direct_rows(level, block):
            at = serial
            serial += 1
            up_src, up_dst = pl.ds(block - rows, rows), pl.ds(halo - (distance - 1) * block - rows, rows)
            down_src, down_dst = pl.ds(0, rows), pl.ds((distance - 1) * block, rows)
            up = remote(own[level].at[up_src], ups[level].at[up_dst], up_send.at[at], up_recv.at[at], me + distance)
            down = remote(
                own[level].at[down_src], downs[level].at[down_dst], down_send.at[at], down_recv.at[at], me - distance)
            up_ok, down_ok = me + distance < devices, me >= distance
            arrivals[level] += [(down_ok, up), (up_ok, down)]
            if distance % 2 == 0:
                starts += [(level, up_ok, up), (level, down_ok, down)]
                sends += [(up_ok, up), (down_ok, down)]
                continue
            up_ok, down_ok = jnp.logical_and(is_odd, up_ok), jnp.logical_and(even, down_ok)
            starts += [(level, up_ok, up), (level, down_ok, down)]
            sends += [(up_ok, up), (down_ok, down)]
            hop = distance - 1
            up2 = remote(
                others[level].at[up_src], ups[level].at[up_dst], up2_send.at[at], up_recv.at[at], me + hop)
            down2 = remote(
                others[level].at[down_src], downs[level].at[down_dst], down2_send.at[at], down_recv.at[at], me - hop)
            up2_ok = jnp.logical_and(is_odd, me + hop < devices)
            down2_ok = jnp.logical_and(even, me >= hop)
            relays[level] += [(up2_ok, up2), (down2_ok, down2)]
            sends += [(up2_ok, up2), (down2_ok, down2)]

    pair_copies, far_copies = {}, {}
    serial = 0
    for level in (SECOND, THIRD, FINE):
        block = blocks[level]
        near = min(block, HALOS[level])
        pair_copies[level], far_copies[level] = [], []
        for row, rows, forwarded in pair_rows(level, block):
            mirrored = block - row - rows
            at = mirrored + odd * (row - mirrored)
            pair_copies[level].append(remote(
                own[level].at[pl.ds(at, rows)], others[level].at[pl.ds(at, rows)],
                pair_send.at[serial], pair_recv.at[serial], partner))
            relay = None
            if forwarded:
                held = row + odd * (mirrored - row)
                spot = block + held - (1 - odd) * (block - near)
                relay = remote(
                    others[level].at[pl.ds(held, rows)], others[level].at[pl.ds(spot, rows)],
                    far_send.at[serial], far_recv.at[serial], target)
            far_copies[level].append(relay)
            serial += 1
        for wanted, ok, copy in starts:
            if wanted == level:
                pl.when(ok)(copy.start)
        for copy in pair_copies[level]:
            copy.start()

    def pass_on(level, chunk):
        pair_copies[level][chunk].wait_recv()
        if far_copies[level][chunk] is not None:
            pl.when(has_target)(far_copies[level][chunk].start)
        for ok, copy in relays.get(level, ()):
            pl.when(ok)(copy.start)

    def arrive(level):
        for ok, copy in arrivals[level]:
            pl.when(ok)(copy.wait_recv)
        for copy in far_copies[level]:
            pl.when(has_source)(copy.wait_recv)

    def inside(level, row):
        block = blocks[level]
        if 0 <= row < block:
            return None
        place = me * block + row
        return jnp.logical_and(place >= 0, place < devices * block)

    def store_padded(ref, at, values, level, first_row):
        steps = values.shape[1]
        for r in range(values.shape[0]):
            row = values[r:r + 1].astype(jnp.float32)
            valid = inside(level, first_row + r)
            if valid is not None:
                row = jnp.where(valid, row, 0.0)
            before, after = edge_steps(row, False)
            line = [before[0]] + [row[0, t] for t in range(steps)] + [after[0]]
            for pair in range(steps // 2):
                d0, d1, d2, d3 = line[2 * pair:2 * pair + 4]
                for kind, value in enumerate((d0 - d2, d1 + d2, d2 - d1, d1 - d3)):
                    ref[at + r, kind, pair] = value.astype(jnp.bfloat16)

    def mix_taps(k):
        weight_copies[k].wait()
        for a in range(3):
            sides = 0.5 * (weights[k, a, 0].astype(jnp.float32) + weights[k, a, 2].astype(jnp.float32))
            middle = 0.5 * weights[k, a, 1].astype(jnp.float32)
            mixed[k, 0, a] = (sides + middle).astype(jnp.bfloat16)
            mixed[k, 1, a] = (sides - middle).astype(jnp.bfloat16)

    def conv(ref, k, tiles, emit):
        half, channels = ref.shape[2], ref.shape[4]
        bias = bias_ref[k:k + 1, :]
        taps = [[weights[k, a, 0] for a in range(3)], [mixed[k, 0, a] for a in range(3)],
                [mixed[k, 1, a] for a in range(3)], [weights[k, a, 2] for a in range(3)]]
        for r, rows in tiles:
            parts = []
            for kind in range(4):
                flat = jnp.concatenate(
                    [ref[r + a:r + a + rows, kind].reshape(rows * half * LANES, channels) for a in range(3)], axis=1)
                parts.append(jnp.dot(
                    flat, jnp.concatenate(taps[kind], axis=0), preferred_element_type=jnp.float32))
            left = bias + parts[0] + parts[1] + parts[2]
            right = bias + parts[1] - parts[2] - parts[3]
            shape = (rows, half, 1, LANES, channels)
            acc = jnp.concatenate([left.reshape(shape), right.reshape(shape)], axis=2)
            emit(r, acc.reshape(rows, 2 * half, LANES, channels))

    def tiles_of(level, first, last):
        return parts_of(first, last, max(1, MOST // own[level].shape[1]))

    def raw_row(level, place):
        block, halo = blocks[level], HALOS[level]
        near = min(block, halo)
        if 0 <= place < block:
            return own[level][place]
        if place < 0:
            j = -1 - place
            if j >= block:
                return ups[level][halo - 1 - j]
            return others[level][block - 1 - j + (1 - odd) * near]
        j = place - block
        if j >= block:
            return downs[level][j]
        return others[level][j + odd * block]

    def take_rows(level, padded, first, last):
        halo = HALOS[level]
        columns = own[level].shape[1]
        steps = columns // LANES
        width = stage.shape[3]
        for place in range(first, last):
            row = raw_row(level, place).astype(jnp.float32)
            slot = place % stage.shape[0]
            parts = range(row.shape[1] // width)
            for c in parts:
                stage[slot, c, 0:columns] = row[:, c * width:(c + 1) * width]
            turned = jnp.concatenate(
                [jnp.concatenate([stage[slot, c, pl.ds(t, LANES, stride=steps), :] for c in parts], axis=1)[None]
                 for t in range(steps)], axis=0)
            fields[level][halo + place] = turned.astype(jnp.bfloat16)
            store_padded(padded, halo + place, jnp.maximum(turned, 0.0)[None], level, place)

    def hidden(level, source, target, k, tiles, row0):
        def emit(r, acc):
            store_padded(target, r, jnp.maximum(acc, 0.0), level, row0 + r)
        conv(source, k, tiles, emit)

    def source_rows(level, row, rows):
        at = HALOS[level] + row
        return fields[level][at:at + rows].astype(jnp.float32)

    def lift(level, refined, halo, index, emit, extra):
        count, steps = refined.shape[0], refined.shape[1]
        block = blocks[level]
        w = projs[index]
        tile = max(1, 512 // (steps * LANES))
        for r in range(0, count, tile):
            rows = min(tile, count - r)
            y = jnp.dot(refined[r:r + rows].reshape(rows * steps * LANES, -1), w,
                        preferred_element_type=jnp.float32)
            proj_y[r:r + rows, 0:steps] = y.reshape(rows, steps, LANES, -1)

        def line(m):
            value = proj_y[m, 0:steps]
            before, after = halo - 1 - m, m - halo - block
            if before >= 0 and before % block == 0:
                value = jnp.where(me == before // block, proj_y[m + 1, 0:steps], value)
            if after >= 0 and after % block == 0:
                value = jnp.where(me == devices - 1 - after // block, proj_y[m - 1, 0:steps], value)
            return value

        bias = proj_bias_ref[index:index + 1, :]

        def columns(out_row, major, minor):
            row = (0.75 * major + 0.25 * minor + bias)[None]
            before, after = edge_steps(row, True)
            wide = jnp.concatenate([before[:, None], row, after[:, None]], axis=1)[0]
            low = 0.25 * wide[0:steps] + 0.75 * row[0]
            high = 0.75 * row[0] + 0.25 * wide[2:steps + 2]
            emit(out_row, low.astype(jnp.bfloat16), high.astype(jnp.bfloat16))

        for m in range(count):
            even = 2 * (m - halo)
            if 1 <= m and (m < count - 1 or extra):
                columns(even, line(m), line(m - 1))
            if m < count - 1 and (m >= 1 or extra):
                columns(even + 1, line(m), line(m + 1))

    def emit_to(ref, first):
        def emit(row, low, high):
            for t in range(low.shape[0]):
                ref[row - first, 2 * t] = low[t]
                ref[row - first, 2 * t + 1] = high[t]
        return emit

    halo_f, halo_s, halo_t = HALOS
    block_f, block_s, block_t = blocks
    order = [row for row, _, _ in pair_rows(FINE, block_f)]

    def fine_unit(tiles):
        def emit(r, acc):
            rows = acc.shape[0]
            addend_f[r:r + rows] = acc + source_rows(FINE, r + 2 - halo_f, rows)
        conv(hidden_f, 7, tiles, emit)

    def fine_join(first, last):
        for r in range(first, last):
            total = (addend_f[r:r + 1] + path_f[r:r + 1].astype(jnp.float32)).astype(jnp.bfloat16)
            merged_f[r:r + 1] = total
            store_padded(joined_f, r, jnp.maximum(total, 0), FINE, r + 2 - halo_f)

    def fine_refined(tiles):
        def emit(r, acc):
            rows = acc.shape[0]
            refined_f[r:r + rows] = (acc + merged_f[r + 2:r + 2 + rows].astype(jnp.float32)).astype(jnp.bfloat16)
        conv(hidden2_f, 9, tiles, emit)

    last_index = projs.shape[0] - 1

    def project(tiles):
        bias = proj_bias_ref[last_index:last_index + 1, :]
        for r, rows in tiles:
            y = jnp.dot(refined_f[r:r + rows].reshape(rows * refined_f.shape[1] * LANES, -1), projs[last_index],
                        preferred_element_type=jnp.float32) + bias
            lines_f[r:r + rows] = y.astype(jnp.bfloat16).reshape(rows, refined_f.shape[1], LANES, -1)

    take_rows(FINE, padded_f, 0, block_f)
    mix_taps(6)
    mix_taps(7)
    hidden(FINE, padded_f, hidden_f, 6, tiles_of(FINE, halo_f, halo_f + block_f - 2), 1 - halo_f)
    fine_unit(tiles_of(FINE, halo_f, halo_f + block_f - 4))
    pass_on(SECOND, 0)
    mix_taps(2)
    take_rows(THIRD, padded_t, 0, block_t)
    take_rows(SECOND, padded_s, 0, block_s)
    for at in range(1, len(pair_copies[SECOND])):
        pass_on(SECOND, at)
    mix_taps(0)
    mix_taps(1)
    mix_taps(3)
    fill_table(table, own[FINE].shape[1])
    pass_on(THIRD, 0)
    for k in (4, 5, 8, 9):
        mix_taps(k)

    last_s = block_s + 2 * halo_s
    arrive(SECOND)
    pass_on(FINE, 0)
    take_rows(SECOND, padded_s, -halo_s, 0)
    take_rows(SECOND, padded_s, block_s, block_s + halo_s)
    hidden(SECOND, padded_s, hidden_s, 2, tiles_of(SECOND, 0, last_s - 2), 1 - halo_s)
    arrive(THIRD)
    pass_on(FINE, 1)
    take_rows(THIRD, padded_t, -halo_t, 0)
    take_rows(THIRD, padded_t, block_t, block_t + halo_t)
    proj_copy.wait()
    hidden(THIRD, padded_t, hidden_t, 0, tiles_of(THIRD, 0, block_t + 2 * halo_t - 2), 1 - halo_t)

    def emit_third(r, acc):
        rows = acc.shape[0]
        total = acc + source_rows(THIRD, r + 2 - halo_t, rows)
        refined_t[r:r + rows] = total.astype(jnp.bfloat16)

    conv(hidden_t, 1, tiles_of(THIRD, 0, block_t + 2 * halo_t - 4), emit_third)
    lift(THIRD, refined_t, halo_t - 2, 0, emit_to(path_s, 2 - halo_s), False)

    def emit_merged(r, acc):
        rows = acc.shape[0]
        total = acc + source_rows(SECOND, r + 2 - halo_s, rows) + path_s[r:r + rows].astype(jnp.float32)
        total = total.astype(jnp.bfloat16)
        merged_s[r:r + rows] = total
        store_padded(padded_s, r, jnp.maximum(total, 0), SECOND, r + 2 - halo_s)

    conv(hidden_s, 3, tiles_of(SECOND, 0, last_s - 4), emit_merged)
    pass_on(FINE, 2)
    pass_on(FINE, 3)

    hidden(SECOND, padded_s, hidden_s, 4, tiles_of(SECOND, 0, last_s - 6), 3 - halo_s)

    def emit_refined(r, acc):
        rows = acc.shape[0]
        total = acc + merged_s[r + 2:r + 2 + rows].astype(jnp.float32)
        refined_s[r:r + rows] = total.astype(jnp.bfloat16)

    conv(hidden_s, 5, tiles_of(SECOND, 0, last_s - 8), emit_refined)
    pass_on(FINE, 4)

    ring = RING
    wide_f = block_f + 2 * halo_f
    far_of = {row: at for at, row in enumerate(order)}
    for d in range(ring):
        pl.when(has_source)(far_copies[FINE][far_of[block_f - 1 - d]].wait_recv)
    lift(SECOND, refined_s, halo_s - 4, 1, emit_to(path_f, 2 - halo_f), True)
    take_rows(FINE, padded_f, -ring, 0)
    take_rows(FINE, padded_f, block_f, block_f + ring)
    hidden(FINE, padded_f, hidden_f, 6, [(halo_f - ring, ring), (halo_f + block_f - 2, ring)], 1 - halo_f)
    fine_unit([(halo_f - ring, ring), (halo_f + block_f - 4, ring)])
    low, high = halo_f - ring, halo_f + block_f - 4 + ring
    pass_on(FINE, 5)
    fine_join(low, high)
    hidden(FINE, joined_f, hidden2_f, 8, tiles_of(FINE, low, high - 2), 3 - halo_f)
    fine_refined(tiles_of(FINE, low, high - 4))
    project(tiles_of(FINE, low, high - 4))

    for at in range(6, len(order)):
        pass_on(FINE, at)
    for at, row in enumerate(order):
        if far_copies[FINE][at] is not None and row < block_f - ring:
            pl.when(has_source)(far_copies[FINE][at].wait_recv)
    take_rows(FINE, padded_f, -halo_f, -ring)
    take_rows(FINE, padded_f, block_f + ring, block_f + halo_f)
    edge = halo_f - ring
    ends = lambda count: [(0, edge), (count - edge, edge)]
    hidden(FINE, padded_f, hidden_f, 6, ends(wide_f - 2), 1 - halo_f)
    fine_unit(ends(wide_f - 4))
    fine_join(0, edge)
    fine_join(wide_f - 4 - edge, wide_f - 4)
    hidden(FINE, joined_f, hidden2_f, 8, ends(wide_f - 6), 3 - halo_f)
    fine_refined(ends(wide_f - 8))
    project(ends(wide_f - 8))
    count = lines_f.shape[0]
    for end, beside, at_end in ((0, 1, me == 0), (count - 1, count - 2, me == devices - 1)):
        lines_f[end] = jnp.where(
            at_end, lines_f[beside].astype(jnp.float32), lines_f[end].astype(jnp.float32)).astype(jnp.bfloat16)

    for ok, copy in sends:
        pl.when(ok)(copy.wait_send)
    for level in (THIRD, SECOND, FINE):
        for copy in pair_copies[level]:
            copy.wait_send()
        for copy in far_copies[level]:
            if copy is not None:
                pl.when(has_target)(copy.wait_send)


def fill_table(table, columns):
    steps = columns // LANES
    wide = 2 * columns
    for half in range(2):
        for side in range(2):
            out = lax.broadcasted_iota(jnp.int32, (wide, columns), 0)
            place = lax.broadcasted_iota(jnp.int32, (wide, columns), 1)
            column = (place % LANES) * steps + place // LANES
            near = out // 2
            far = jnp.clip(near + 2 * (out % 2) - 1, 0, columns - 1)
            weight = jnp.where(column == near, 0.75, 0.0) + jnp.where(column == far, 0.25, 0.0)
            weight = weight * (0.75 if half == side else 0.25)
            table[half * wide:(half + 1) * wide, side * columns:(side + 1) * columns] = weight.astype(jnp.bfloat16)


def lift_kernel(lines_ref, table_ref, out_ref):
    at = pl.program_id(0)
    steps, channels = lines_ref.shape[1], lines_ref.shape[3]
    columns = steps * LANES
    wide = 2 * columns
    per = out_ref.shape[0] // 2
    for i in range(per + 1):
        pair = lines_ref[pl.ds(at * per + i, 2)].reshape(2 * columns, channels)
        first, last = (wide if i == 0 else 0), (wide if i == per else 2 * wide)
        rows = jnp.dot(table_ref[first:last], pair, preferred_element_type=jnp.float32).astype(jnp.bfloat16)
        if i > 0:
            out_ref[2 * i - 1] = rows[0:wide]
        if i < per:
            out_ref[2 * i] = rows[last - first - wide:]


def local(devices, feat_fine, feat_second, feat_third, conv_weight, conv_bias, out_weight, out_bias):
    fields = (feat_fine, feat_second, feat_third)
    channels = feat_fine.shape[2]
    blocks = [v.shape[0] for v in fields]
    columns = [v.shape[1] for v in fields]
    steps = [c // LANES for c in columns]
    width = min(128, channels)

    def raw(count, level):
        return pltpu.VMEM((count, columns[level], channels), jnp.bfloat16)

    def rows_of(count, level, dtype=jnp.bfloat16):
        return pltpu.VMEM((count, steps[level], LANES, channels), dtype)

    def mixed_rows(count, level):
        return pltpu.VMEM((count, 4, steps[level] // 2, LANES, channels), jnp.bfloat16)

    extents = [block + 2 * halo for block, halo in zip(blocks, HALOS)]
    copies = sum(len(direct_rows(level, blocks[level])) for level in (SECOND, THIRD))
    pairs = sum(len(pair_rows(level, blocks[level])) for level in range(3))
    dma = pltpu.SemaphoreType.DMA
    scratch = [raw(blocks[level], level) for level in range(3)]
    scratch += [pltpu.VMEM(conv_bias.shape, jnp.float32), pltpu.VMEM(out_bias.shape, jnp.float32)]
    for level in range(3):
        scratch += [raw(blocks[level] + min(blocks[level], HALOS[level]), level)]
    scratch += [raw(HALOS[level], level) for level in (SECOND, THIRD) for _ in range(2)]
    scratch += [rows_of(extents[level], level) for level in range(3)]
    scratch += [pltpu.VMEM((8, channels // width, columns[FINE], width), jnp.float32)]
    convs = conv_weight.shape[0]
    scratch += [pltpu.VMEM((convs, 3, 3, channels, channels), jnp.bfloat16),
                pltpu.VMEM((convs, 2, 3, channels, channels), jnp.bfloat16),
                pltpu.VMEM(out_weight.shape, jnp.bfloat16)]
    scratch += [mixed_rows(extents[FINE], FINE), mixed_rows(extents[FINE] - 2, FINE),
                rows_of(extents[FINE] - 4, FINE, jnp.float32), mixed_rows(extents[FINE] - 4, FINE),
                mixed_rows(extents[FINE] - 6, FINE), rows_of(extents[FINE] - 4, FINE), rows_of(extents[FINE] - 4, FINE)]
    scratch += [mixed_rows(extents[SECOND], SECOND), mixed_rows(extents[SECOND] - 2, SECOND),
                rows_of(extents[SECOND] - 4, SECOND), rows_of(extents[SECOND] - 4, SECOND)]
    scratch += [mixed_rows(extents[THIRD], THIRD), mixed_rows(extents[THIRD] - 2, THIRD)]
    scratch += [rows_of(extents[FINE] - 8, FINE), rows_of(extents[SECOND] - 8, SECOND),
                rows_of(extents[THIRD] - 4, THIRD)]
    scratch += [rows_of(max(extents[SECOND] - 8, extents[THIRD] - 4), SECOND, jnp.float32)]
    scratch += [dma((copies,)) for _ in range(6)] + [dma((pairs,)) for _ in range(4)]
    scratch += [dma((conv_weight.shape[0],)), dma, dma((5,))]
    vmem, far = pl.BlockSpec(memory_space=pltpu.VMEM), pl.BlockSpec(memory_space=pltpu.HBM)
    wide = 2 * columns[FINE]
    lines, table = pl.pallas_call(
        functools.partial(kernel, devices),
        out_shape=[jax.ShapeDtypeStruct((extents[FINE] - 8, steps[FINE], LANES, channels), jnp.bfloat16),
                   jax.ShapeDtypeStruct((2 * wide, 2 * columns[FINE]), jnp.bfloat16)],
        in_specs=[far] * 7,
        out_specs=[vmem, vmem],
        scratch_shapes=scratch,
        compiler_params=pltpu.CompilerParams(
            collective_id=0, has_side_effects=True, vmem_limit_bytes=VMEM_MIB * 1024 * 1024),
    )(*[pltpu.with_memory_space_constraint(v, pltpu.HBM) for v in (
        *fields, conv_weight.reshape(convs, 3, 3, channels, channels), conv_bias, out_weight, out_bias)])
    per = 2 if blocks[FINE] % 2 == 0 else 1
    return pl.pallas_call(
        lift_kernel,
        grid=(blocks[FINE] // per,),
        out_shape=jax.ShapeDtypeStruct((2 * blocks[FINE], wide, channels), jnp.bfloat16),
        in_specs=[vmem, vmem],
        out_specs=pl.BlockSpec((2 * per, wide, channels), lambda g: (g, 0, 0)),
        compiler_params=pltpu.CompilerParams(vmem_limit_bytes=8 * 1024 * 1024),
    )(lines, table)


def solution(mesh):
    rows = P(("img", "rows"), None, None)
    return jax.shard_map(
        functools.partial(local, mesh.shape["rows"]),
        mesh=mesh,
        in_specs=(rows, rows, rows, P(), P(), P(), P()),
        out_specs=rows,
        check_vma=False,
    )
```

```python
import functools

import jax
import jax.numpy as jnp
from jax import lax
from jax.experimental import pallas as pl
from jax.experimental.pallas import tpu as pltpu
from jax.sharding import PartitionSpec as P

MESH = pl.DeviceIdType.MESH
LANES = 16
VMEM_MIB = 52
MOST = 640
RING = 1
FINE, SECOND, THIRD = 0, 1, 2
HALOS = (5, 6, 5)
WEIGHT_ORDER = (6, 7, 2, 0, 1, 3, 4, 5, 8, 9)


def direct_rows(level, block):
    halo = HALOS[level]
    return [(d, min(block, halo - (d - 1) * block)) for d in range(2, -(-halo // block) + 1)]


def pair_rows(level, block):
    near = min(block, HALOS[level])
    if level == THIRD:
        return [(0, block, True)]
    if level == SECOND:
        cuts = [block, block // 2, 0] if block > 1 else [block, 0]
        return [(low, high - low, True) for high, low in zip(cuts, cuts[1:])]
    away, beside = list(range(block - 1, -1, -1)), list(range(block))
    order = away[:2] + beside[:RING] + away[2:near]
    order = list(dict.fromkeys(order + beside[:near] + away))
    return [(r, 1, r >= block - near) for r in order]


def parts_of(first, last, most):
    rows = last - first
    parts = -(-rows // most)
    cuts = [first + rows * i // parts for i in range(parts + 1)]
    return [(p, q - p) for p, q in zip(cuts, cuts[1:])]


def edge_steps(values, clamp):
    steps = values.shape[1]
    first, last = values[:, 0], values[:, steps - 1]
    place = lax.broadcasted_iota(jnp.int32, first.shape, 1)
    zero = jnp.zeros_like(first)
    before = jnp.where(place == 0, first if clamp else zero, pltpu.roll(last, 1, 1))
    after = jnp.where(place == LANES - 1, last if clamp else zero, pltpu.roll(first, LANES - 1, 1))
    return before, after


def kernel(
    devices, fine_hbm, second_hbm, third_hbm, conv_hbm, bias_hbm, proj_hbm, proj_bias_hbm, lines_f, table,
    fine_ref, second_ref, third_ref, bias_ref, proj_bias_ref,
    fine_other, second_other, third_other,
    second_up, second_down, third_up, third_down,
    fine_x, second_x, third_x, stage, weights, mixed, projs,
    padded_f, hidden_f, addend_f, joined_f, hidden2_f, merged_f, path_f,
    padded_s, hidden_s, merged_s, path_s,
    padded_t, hidden_t, refined_f, refined_s, refined_t, proj_y,
    up_send, up_recv, down_send, down_recv, up2_send, down2_send,
    pair_send, pair_recv, far_send, far_recv, weight_sem, proj_sem, in_sem,
):
    me = lax.axis_index("rows")
    own = (fine_ref, second_ref, third_ref)
    ups = (None, second_up, third_up)
    downs = (None, second_down, third_down)
    blocks = tuple(ref.shape[0] for ref in own)
    fields = (fine_x, second_x, third_x)
    others = (fine_other, second_other, third_other)
    odd = me % 2
    even = odd == 0
    is_odd = odd == 1
    partner = me + 1 - 2 * odd
    target = me + 2 - 4 * odd
    source = me - 2 + 4 * odd

    in_copies = [
        pltpu.make_async_copy(source_ref, into, in_sem.at[at])
        for at, (source_ref, into) in enumerate((
            (second_hbm, second_ref), (third_hbm, third_ref), (fine_hbm, fine_ref),
            (bias_hbm, bias_ref), (proj_bias_hbm, proj_bias_ref)))
    ]
    for copy in in_copies:
        copy.start()
    weight_copies = {
        k: pltpu.make_async_copy(conv_hbm.at[k], weights.at[k], weight_sem.at[k])
        for k in WEIGHT_ORDER
    }
    proj_copy = pltpu.make_async_copy(proj_hbm, projs, proj_sem)
    for at, k in enumerate(WEIGHT_ORDER):
        weight_copies[k].start()
        if at == 3:
            proj_copy.start()

    reach = max([2] + [d for level in (SECOND, THIRD) for d, _ in direct_rows(level, blocks[level])])
    barrier = pltpu.get_barrier_semaphore()
    for distance in range(1, reach + 1):
        @pl.when(me >= distance)
        def _():
            pl.semaphore_signal(barrier, inc=1, device_id={"rows": me - distance}, device_id_type=MESH)

        @pl.when(me + distance < devices)
        def _():
            pl.semaphore_signal(barrier, inc=1, device_id={"rows": me + distance}, device_id_type=MESH)
    expected = jnp.minimum(me, reach) + jnp.minimum(devices - 1 - me, reach)
    pl.semaphore_wait(barrier, expected)
    for copy in in_copies:
        copy.wait()

    has_target = jnp.logical_and(target >= 0, target < devices)
    has_source = jnp.logical_and(source >= 0, source < devices)

    def remote(src, dst, send, recv, device):
        return pltpu.make_async_remote_copy(
            src_ref=src, dst_ref=dst, send_sem=send, recv_sem=recv,
            device_id={"rows": device}, device_id_type=MESH)

    starts, sends, arrivals, relays = [], [], {THIRD: [], SECOND: []}, {THIRD: [], SECOND: []}
    serial = 0
    for level in (THIRD, SECOND):
        block, halo = blocks[level], HALOS[level]
        for distance, rows in direct_rows(level, block):
            at = serial
            serial += 1
            up_src, up_dst = pl.ds(block - rows, rows), pl.ds(halo - (distance - 1) * block - rows, rows)
            down_src, down_dst = pl.ds(0, rows), pl.ds((distance - 1) * block, rows)
            up = remote(own[level].at[up_src], ups[level].at[up_dst], up_send.at[at], up_recv.at[at], me + distance)
            down = remote(
                own[level].at[down_src], downs[level].at[down_dst], down_send.at[at], down_recv.at[at], me - distance)
            up_ok, down_ok = me + distance < devices, me >= distance
            arrivals[level] += [(down_ok, up), (up_ok, down)]
            if distance % 2 == 0:
                starts += [(level, up_ok, up), (level, down_ok, down)]
                sends += [(up_ok, up), (down_ok, down)]
                continue
            up_ok, down_ok = jnp.logical_and(is_odd, up_ok), jnp.logical_and(even, down_ok)
            starts += [(level, up_ok, up), (level, down_ok, down)]
            sends += [(up_ok, up), (down_ok, down)]
            hop = distance - 1
            up2 = remote(
                others[level].at[up_src], ups[level].at[up_dst], up2_send.at[at], up_recv.at[at], me + hop)
            down2 = remote(
                others[level].at[down_src], downs[level].at[down_dst], down2_send.at[at], down_recv.at[at], me - hop)
            up2_ok = jnp.logical_and(is_odd, me + hop < devices)
            down2_ok = jnp.logical_and(even, me >= hop)
            relays[level] += [(up2_ok, up2), (down2_ok, down2)]
            sends += [(up2_ok, up2), (down2_ok, down2)]

    pair_copies, far_copies = {}, {}
    serial = 0
    for level in (SECOND, THIRD, FINE):
        block = blocks[level]
        near = min(block, HALOS[level])
        pair_copies[level], far_copies[level] = [], []
        for row, rows, forwarded in pair_rows(level, block):
            mirrored = block - row - rows
            at = mirrored + odd * (row - mirrored)
            pair_copies[level].append(remote(
                own[level].at[pl.ds(at, rows)], others[level].at[pl.ds(at, rows)],
                pair_send.at[serial], pair_recv.at[serial], partner))
            relay = None
            if forwarded:
                held = row + odd * (mirrored - row)
                spot = block + held - (1 - odd) * (block - near)
                relay = remote(
                    others[level].at[pl.ds(held, rows)], others[level].at[pl.ds(spot, rows)],
                    far_send.at[serial], far_recv.at[serial], target)
            far_copies[level].append(relay)
            serial += 1
        for wanted, ok, copy in starts:
            if wanted == level:
                pl.when(ok)(copy.start)
        for copy in pair_copies[level]:
            copy.start()

    def pass_on(level, chunk):
        pair_copies[level][chunk].wait_recv()
        if far_copies[level][chunk] is not None:
            pl.when(has_target)(far_copies[level][chunk].start)
        for ok, copy in relays.get(level, ()):
            pl.when(ok)(copy.start)

    def arrive(level):
        for ok, copy in arrivals[level]:
            pl.when(ok)(copy.wait_recv)
        for copy in far_copies[level]:
            pl.when(has_source)(copy.wait_recv)

    def inside(level, row):
        block = blocks[level]
        if 0 <= row < block:
            return None
        place = me * block + row
        return jnp.logical_and(place >= 0, place < devices * block)

    def store_padded(ref, at, values, level, first_row):
        steps = values.shape[1]
        for r in range(values.shape[0]):
            row = values[r:r + 1].astype(jnp.float32)
            valid = inside(level, first_row + r)
            if valid is not None:
                row = jnp.where(valid, row, 0.0)
            before, after = edge_steps(row, False)
            line = [before[0]] + [row[0, t] for t in range(steps)] + [after[0]]
            for pair in range(steps // 2):
                d0, d1, d2, d3 = line[2 * pair:2 * pair + 4]
                for kind, value in enumerate((d0 - d2, d1 + d2, d2 - d1, d1 - d3)):
                    ref[at + r, kind, pair] = value.astype(jnp.bfloat16)

    def mix_taps(k):
        weight_copies[k].wait()
        for a in range(3):
            sides = 0.5 * (weights[k, a, 0].astype(jnp.float32) + weights[k, a, 2].astype(jnp.float32))
            middle = 0.5 * weights[k, a, 1].astype(jnp.float32)
            mixed[k, 0, a] = (sides + middle).astype(jnp.bfloat16)
            mixed[k, 1, a] = (sides - middle).astype(jnp.bfloat16)

    def conv(ref, k, tiles, emit):
        half, channels = ref.shape[2], ref.shape[4]
        bias = bias_ref[k:k + 1, :]
        taps = [[weights[k, a, 0] for a in range(3)], [mixed[k, 0, a] for a in range(3)],
                [mixed[k, 1, a] for a in range(3)], [weights[k, a, 2] for a in range(3)]]
        for r, rows in tiles:
            parts = []
            for kind in range(4):
                flat = jnp.concatenate(
                    [ref[r + a:r + a + rows, kind].reshape(rows * half * LANES, channels) for a in range(3)], axis=1)
                parts.append(jnp.dot(
                    flat, jnp.concatenate(taps[kind], axis=0), preferred_element_type=jnp.float32))
            left = bias + parts[0] + parts[1] + parts[2]
            right = bias + parts[1] - parts[2] - parts[3]
            shape = (rows, half, 1, LANES, channels)
            acc = jnp.concatenate([left.reshape(shape), right.reshape(shape)], axis=2)
            emit(r, acc.reshape(rows, 2 * half, LANES, channels))

    def tiles_of(level, first, last):
        return parts_of(first, last, max(1, MOST // own[level].shape[1]))

    def raw_row(level, place):
        block, halo = blocks[level], HALOS[level]
        near = min(block, halo)
        if 0 <= place < block:
            return own[level][place]
        if place < 0:
            j = -1 - place
            if j >= block:
                return ups[level][halo - 1 - j]
            return others[level][block - 1 - j + (1 - odd) * near]
        j = place - block
        if j >= block:
            return downs[level][j]
        return others[level][j + odd * block]

    def take_rows(level, padded, first, last):
        halo = HALOS[level]
        columns = own[level].shape[1]
        steps = columns // LANES
        width = stage.shape[3]
        for place in range(first, last):
            row = raw_row(level, place).astype(jnp.float32)
            slot = place % stage.shape[0]
            parts = range(row.shape[1] // width)
            for c in parts:
                stage[slot, c, 0:columns] = row[:, c * width:(c + 1) * width]
            turned = jnp.concatenate(
                [jnp.concatenate([stage[slot, c, pl.ds(t, LANES, stride=steps), :] for c in parts], axis=1)[None]
                 for t in range(steps)], axis=0)
            fields[level][halo + place] = turned.astype(jnp.bfloat16)
            store_padded(padded, halo + place, jnp.maximum(turned, 0.0)[None], level, place)

    def hidden(level, source, target, k, tiles, row0):
        def emit(r, acc):
            store_padded(target, r, jnp.maximum(acc, 0.0), level, row0 + r)
        conv(source, k, tiles, emit)

    def source_rows(level, row, rows):
        at = HALOS[level] + row
        return fields[level][at:at + rows].astype(jnp.float32)

    def lift(level, refined, halo, index, emit, extra):
        count, steps = refined.shape[0], refined.shape[1]
        block = blocks[level]
        w = projs[index]
        tile = max(1, 512 // (steps * LANES))
        for r in range(0, count, tile):
            rows = min(tile, count - r)
            y = jnp.dot(refined[r:r + rows].reshape(rows * steps * LANES, -1), w,
                        preferred_element_type=jnp.float32)
            proj_y[r:r + rows, 0:steps] = y.reshape(rows, steps, LANES, -1)

        def line(m):
            value = proj_y[m, 0:steps]
            before, after = halo - 1 - m, m - halo - block
            if before >= 0 and before % block == 0:
                value = jnp.where(me == before // block, proj_y[m + 1, 0:steps], value)
            if after >= 0 and after % block == 0:
                value = jnp.where(me == devices - 1 - after // block, proj_y[m - 1, 0:steps], value)
            return value

        bias = proj_bias_ref[index:index + 1, :]

        def columns(out_row, major, minor):
            row = (0.75 * major + 0.25 * minor + bias)[None]
            before, after = edge_steps(row, True)
            wide = jnp.concatenate([before[:, None], row, after[:, None]], axis=1)[0]
            low = 0.25 * wide[0:steps] + 0.75 * row[0]
            high = 0.75 * row[0] + 0.25 * wide[2:steps + 2]
            emit(out_row, low.astype(jnp.bfloat16), high.astype(jnp.bfloat16))

        for m in range(count):
            even = 2 * (m - halo)
            if 1 <= m and (m < count - 1 or extra):
                columns(even, line(m), line(m - 1))
            if m < count - 1 and (m >= 1 or extra):
                columns(even + 1, line(m), line(m + 1))

    def emit_to(ref, first):
        def emit(row, low, high):
            for t in range(low.shape[0]):
                ref[row - first, 2 * t] = low[t]
                ref[row - first, 2 * t + 1] = high[t]
        return emit

    halo_f, halo_s, halo_t = HALOS
    block_f, block_s, block_t = blocks
    order = [row for row, _, _ in pair_rows(FINE, block_f)]

    def fine_unit(tiles):
        def emit(r, acc):
            rows = acc.shape[0]
            addend_f[r:r + rows] = acc + source_rows(FINE, r + 2 - halo_f, rows)
        conv(hidden_f, 7, tiles, emit)

    def fine_join(first, last):
        for r in range(first, last):
            total = (addend_f[r:r + 1] + path_f[r:r + 1].astype(jnp.float32)).astype(jnp.bfloat16)
            merged_f[r:r + 1] = total
            store_padded(joined_f, r, jnp.maximum(total, 0), FINE, r + 2 - halo_f)

    def fine_refined(tiles):
        def emit(r, acc):
            rows = acc.shape[0]
            refined_f[r:r + rows] = (acc + merged_f[r + 2:r + 2 + rows].astype(jnp.float32)).astype(jnp.bfloat16)
        conv(hidden2_f, 9, tiles, emit)

    last_index = projs.shape[0] - 1

    def project(tiles):
        bias = proj_bias_ref[last_index:last_index + 1, :]
        for r, rows in tiles:
            y = jnp.dot(refined_f[r:r + rows].reshape(rows * refined_f.shape[1] * LANES, -1), projs[last_index],
                        preferred_element_type=jnp.float32) + bias
            lines_f[r:r + rows] = y.astype(jnp.bfloat16).reshape(rows, refined_f.shape[1], LANES, -1)

    take_rows(FINE, padded_f, 0, block_f)
    mix_taps(6)
    mix_taps(7)
    hidden(FINE, padded_f, hidden_f, 6, tiles_of(FINE, halo_f, halo_f + block_f - 2), 1 - halo_f)
    fine_unit(tiles_of(FINE, halo_f, halo_f + block_f - 4))
    pass_on(SECOND, 0)
    mix_taps(2)
    take_rows(THIRD, padded_t, 0, block_t)
    take_rows(SECOND, padded_s, 0, block_s)
    for at in range(1, len(pair_copies[SECOND])):
        pass_on(SECOND, at)
    mix_taps(0)
    mix_taps(1)
    mix_taps(3)
    fill_table(table, own[FINE].shape[1])
    pass_on(THIRD, 0)
    for k in (4, 5, 8, 9):
        mix_taps(k)

    last_s = block_s + 2 * halo_s
    arrive(SECOND)
    pass_on(FINE, 0)
    take_rows(SECOND, padded_s, -halo_s, 0)
    take_rows(SECOND, padded_s, block_s, block_s + halo_s)
    hidden(SECOND, padded_s, hidden_s, 2, tiles_of(SECOND, 0, last_s - 2), 1 - halo_s)
    arrive(THIRD)
    pass_on(FINE, 1)
    take_rows(THIRD, padded_t, -halo_t, 0)
    take_rows(THIRD, padded_t, block_t, block_t + halo_t)
    proj_copy.wait()
    hidden(THIRD, padded_t, hidden_t, 0, tiles_of(THIRD, 0, block_t + 2 * halo_t - 2), 1 - halo_t)

    def emit_third(r, acc):
        rows = acc.shape[0]
        total = acc + source_rows(THIRD, r + 2 - halo_t, rows)
        refined_t[r:r + rows] = total.astype(jnp.bfloat16)

    conv(hidden_t, 1, tiles_of(THIRD, 0, block_t + 2 * halo_t - 4), emit_third)
    lift(THIRD, refined_t, halo_t - 2, 0, emit_to(path_s, 2 - halo_s), False)

    def emit_merged(r, acc):
        rows = acc.shape[0]
        total = acc + source_rows(SECOND, r + 2 - halo_s, rows) + path_s[r:r + rows].astype(jnp.float32)
        total = total.astype(jnp.bfloat16)
        merged_s[r:r + rows] = total
        store_padded(padded_s, r, jnp.maximum(total, 0), SECOND, r + 2 - halo_s)

    conv(hidden_s, 3, tiles_of(SECOND, 0, last_s - 4), emit_merged)
    pass_on(FINE, 2)
    pass_on(FINE, 3)

    hidden(SECOND, padded_s, hidden_s, 4, tiles_of(SECOND, 0, last_s - 6), 3 - halo_s)

    def emit_refined(r, acc):
        rows = acc.shape[0]
        total = acc + merged_s[r + 2:r + 2 + rows].astype(jnp.float32)
        refined_s[r:r + rows] = total.astype(jnp.bfloat16)

    conv(hidden_s, 5, tiles_of(SECOND, 0, last_s - 8), emit_refined)
    pass_on(FINE, 4)

    ring = RING
    wide_f = block_f + 2 * halo_f
    far_of = {row: at for at, row in enumerate(order)}
    for d in range(ring):
        pl.when(has_source)(far_copies[FINE][far_of[block_f - 1 - d]].wait_recv)
    lift(SECOND, refined_s, halo_s - 4, 1, emit_to(path_f, 2 - halo_f), True)
    take_rows(FINE, padded_f, -ring, 0)
    take_rows(FINE, padded_f, block_f, block_f + ring)
    hidden(FINE, padded_f, hidden_f, 6, [(halo_f - ring, ring), (halo_f + block_f - 2, ring)], 1 - halo_f)
    fine_unit([(halo_f - ring, ring), (halo_f + block_f - 4, ring)])
    low, high = halo_f - ring, halo_f + block_f - 4 + ring
    pass_on(FINE, 5)
    fine_join(low, high)
    hidden(FINE, joined_f, hidden2_f, 8, tiles_of(FINE, low, high - 2), 3 - halo_f)
    fine_refined(tiles_of(FINE, low, high - 4))
    project(tiles_of(FINE, low, high - 4))

    for at in range(6, len(order)):
        pass_on(FINE, at)
    for at, row in enumerate(order):
        if far_copies[FINE][at] is not None and row < block_f - ring:
            pl.when(has_source)(far_copies[FINE][at].wait_recv)
    take_rows(FINE, padded_f, -halo_f, -ring)
    take_rows(FINE, padded_f, block_f + ring, block_f + halo_f)
    edge = halo_f - ring
    ends = lambda count: [(0, edge), (count - edge, edge)]
    hidden(FINE, padded_f, hidden_f, 6, ends(wide_f - 2), 1 - halo_f)
    fine_unit(ends(wide_f - 4))
    fine_join(0, edge)
    fine_join(wide_f - 4 - edge, wide_f - 4)
    hidden(FINE, joined_f, hidden2_f, 8, ends(wide_f - 6), 3 - halo_f)
    fine_refined(ends(wide_f - 8))
    project(ends(wide_f - 8))
    count = lines_f.shape[0]
    for end, beside, at_end in ((0, 1, me == 0), (count - 1, count - 2, me == devices - 1)):
        lines_f[end] = jnp.where(
            at_end, lines_f[beside].astype(jnp.float32), lines_f[end].astype(jnp.float32)).astype(jnp.bfloat16)

    for ok, copy in sends:
        pl.when(ok)(copy.wait_send)
    for level in (THIRD, SECOND, FINE):
        for copy in pair_copies[level]:
            copy.wait_send()
        for copy in far_copies[level]:
            if copy is not None:
                pl.when(has_target)(copy.wait_send)


def fill_table(table, columns):
    steps = columns // LANES
    wide = 2 * columns
    for half in range(2):
        for side in range(2):
            out = lax.broadcasted_iota(jnp.int32, (wide, columns), 0)
            place = lax.broadcasted_iota(jnp.int32, (wide, columns), 1)
            column = (place % LANES) * steps + place // LANES
            near = out // 2
            far = jnp.clip(near + 2 * (out % 2) - 1, 0, columns - 1)
            weight = jnp.where(column == near, 0.75, 0.0) + jnp.where(column == far, 0.25, 0.0)
            weight = weight * (0.75 if half == side else 0.25)
            table[half * wide:(half + 1) * wide, side * columns:(side + 1) * columns] = weight.astype(jnp.bfloat16)


def lift_kernel(lines_ref, table_ref, out_hbm, rows_ref, sems):
    count, steps, channels = lines_ref.shape[0], lines_ref.shape[1], lines_ref.shape[3]
    columns = steps * LANES
    wide = 2 * columns
    pairs = count - 1
    sent, copies = 0, []
    for i in range(pairs):
        pair = lines_ref[i:i + 2].reshape(2 * columns, channels)
        first, last = (wide if i == 0 else 0), (wide if i == pairs - 1 else 2 * wide)
        rows = jnp.dot(table_ref[first:last], pair, preferred_element_type=jnp.float32).astype(jnp.bfloat16)
        if i > 0:
            rows_ref[2 * i - 1] = rows[0:wide]
        if i < pairs - 1:
            rows_ref[2 * i] = rows[last - first - wide:]
        ready = min(2 * i + 1, 2 * pairs - 2)
        if i in (2 * pairs // 3, pairs - 1) and ready > sent:
            part = pl.ds(sent, ready - sent)
            copies.append(pltpu.make_async_copy(rows_ref.at[part], out_hbm.at[part], sems.at[len(copies)]))
            copies[-1].start()
            sent = ready
    for copy in copies:
        copy.wait()


def local(devices, feat_fine, feat_second, feat_third, conv_weight, conv_bias, out_weight, out_bias):
    fields = (feat_fine, feat_second, feat_third)
    channels = feat_fine.shape[2]
    blocks = [v.shape[0] for v in fields]
    columns = [v.shape[1] for v in fields]
    steps = [c // LANES for c in columns]
    width = min(128, channels)

    def raw(count, level):
        return pltpu.VMEM((count, columns[level], channels), jnp.bfloat16)

    def rows_of(count, level, dtype=jnp.bfloat16):
        return pltpu.VMEM((count, steps[level], LANES, channels), dtype)

    def mixed_rows(count, level):
        return pltpu.VMEM((count, 4, steps[level] // 2, LANES, channels), jnp.bfloat16)

    extents = [block + 2 * halo for block, halo in zip(blocks, HALOS)]
    copies = sum(len(direct_rows(level, blocks[level])) for level in (SECOND, THIRD))
    pairs = sum(len(pair_rows(level, blocks[level])) for level in range(3))
    dma = pltpu.SemaphoreType.DMA
    scratch = [raw(blocks[level], level) for level in range(3)]
    scratch += [pltpu.VMEM(conv_bias.shape, jnp.float32), pltpu.VMEM(out_bias.shape, jnp.float32)]
    for level in range(3):
        scratch += [raw(blocks[level] + min(blocks[level], HALOS[level]), level)]
    scratch += [raw(HALOS[level], level) for level in (SECOND, THIRD) for _ in range(2)]
    scratch += [rows_of(extents[level], level) for level in range(3)]
    scratch += [pltpu.VMEM((8, channels // width, columns[FINE], width), jnp.float32)]
    convs = conv_weight.shape[0]
    scratch += [pltpu.VMEM((convs, 3, 3, channels, channels), jnp.bfloat16),
                pltpu.VMEM((convs, 2, 3, channels, channels), jnp.bfloat16),
                pltpu.VMEM(out_weight.shape, jnp.bfloat16)]
    scratch += [mixed_rows(extents[FINE], FINE), mixed_rows(extents[FINE] - 2, FINE),
                rows_of(extents[FINE] - 4, FINE, jnp.float32), mixed_rows(extents[FINE] - 4, FINE),
                mixed_rows(extents[FINE] - 6, FINE), rows_of(extents[FINE] - 4, FINE), rows_of(extents[FINE] - 4, FINE)]
    scratch += [mixed_rows(extents[SECOND], SECOND), mixed_rows(extents[SECOND] - 2, SECOND),
                rows_of(extents[SECOND] - 4, SECOND), rows_of(extents[SECOND] - 4, SECOND)]
    scratch += [mixed_rows(extents[THIRD], THIRD), mixed_rows(extents[THIRD] - 2, THIRD)]
    scratch += [rows_of(extents[FINE] - 8, FINE), rows_of(extents[SECOND] - 8, SECOND),
                rows_of(extents[THIRD] - 4, THIRD)]
    scratch += [rows_of(max(extents[SECOND] - 8, extents[THIRD] - 4), SECOND, jnp.float32)]
    scratch += [dma((copies,)) for _ in range(6)] + [dma((pairs,)) for _ in range(4)]
    scratch += [dma((conv_weight.shape[0],)), dma, dma((5,))]
    vmem, far = pl.BlockSpec(memory_space=pltpu.VMEM), pl.BlockSpec(memory_space=pltpu.HBM)
    wide = 2 * columns[FINE]
    lines, table = pl.pallas_call(
        functools.partial(kernel, devices),
        out_shape=[jax.ShapeDtypeStruct((extents[FINE] - 8, steps[FINE], LANES, channels), jnp.bfloat16),
                   jax.ShapeDtypeStruct((2 * wide, 2 * columns[FINE]), jnp.bfloat16)],
        in_specs=[far] * 7,
        out_specs=[vmem, vmem],
        scratch_shapes=scratch,
        compiler_params=pltpu.CompilerParams(
            collective_id=0, has_side_effects=True, vmem_limit_bytes=VMEM_MIB * 1024 * 1024),
    )(*[pltpu.with_memory_space_constraint(v, pltpu.HBM) for v in (
        *fields, conv_weight.reshape(convs, 3, 3, channels, channels), conv_bias, out_weight, out_bias)])
    shape = (2 * blocks[FINE], wide, channels)
    return pl.pallas_call(
        lift_kernel,
        out_shape=jax.ShapeDtypeStruct(shape, jnp.bfloat16),
        in_specs=[vmem, vmem],
        out_specs=far,
        scratch_shapes=[pltpu.VMEM(shape, jnp.bfloat16), dma((2,))],
        compiler_params=pltpu.CompilerParams(vmem_limit_bytes=8 * 1024 * 1024),
    )(lines, table)


def solution(mesh):
    rows = P(("img", "rows"), None, None)
    return jax.shard_map(
        functools.partial(local, mesh.shape["rows"]),
        mesh=mesh,
        in_specs=(rows, rows, rows, P(), P(), P(), P()),
        out_specs=rows,
        check_vma=False,
    )
```
